256 devices in a mesh: node: 32 (over y_lo, z, core), local: 8 (over y_hi, x).
Axes of the slice: x: 4, y: 4 (y_hi: 2, y_lo: 2; y = y_hi * 2 + y_lo), z: 8, core: 2. Of those that a mesh axis runs over, the one named last changes fastest.
Arguments:
- activations: bfloat16 [32768, 4096], P(('node', 'local')), may hold values from -24 to 24
- out_grads: bfloat16 [32768, 512], P(('node', 'local')), may hold values from -6 to 6
- master: float32 [4096, 512], P(('node', 'local')), may hold values from -0.15 to 0.15
- first_moment: float32 [4096, 512], P(('node', 'local')), may hold values from -0.6 to 0.6
- second_moment: float32 [4096, 512], P(('node', 'local')), may hold values from 0.01 to 1
Outputs:
- new_weight: bfloat16 [4096, 512], P('node')
- new_first: float32 [4096, 512], P(('node', 'local'))
- new_second: float32 [4096, 512], P(('node', 'local'))
The draws below stay inside these ranges and needn't reach their ends.
All inputs are finite; a program needn't handle non-finite values.
Results may differ from the reference program's by a relative error of at most 0.009.
Values may be sent and summed in bfloat16 or wider, within the bound.
A program may use at most 128 MiB of HBM per device.

```python
import math
import jax
import jax.numpy as jnp
from jax import lax

D = 4096
BLOCK = 256
TOK_DEV = 128
KV = 512
TOKENS = 32768
N_NODE = 32
N_LOCAL = 8


def spiked(drawn, stream_key, source, target, parts, factor):
    owner, partner = [(jnp.arange(drawn.shape[dim]) // (drawn.shape[dim] // parts)).reshape([-1 if axis == dim else 1 for axis in range(drawn.ndim)]) for dim in (source, target)]
    chosen = jax.random.permutation(stream_key, parts)[partner]
    strong = (owner == chosen) | (owner == (partner + parts // 2) % parts)
    return jnp.where(strong, factor * drawn, drawn)


def block_scale(rng, dims, split, least, high):
    level, own = 1.0, jax.random.fold_in(rng, 6)
    for position, blocks in split:
        heights = jnp.exp(jax.random.uniform(jax.random.fold_in(own, position), (blocks,), jnp.float32, least / len(split), high / len(split)))
        level = level * jnp.repeat(heights, dims[position] // blocks).reshape([-1 if axis == position else 1 for axis in range(len(dims))])
    return level


def centred(own_key, shape, width, most, pieces=(), held_as=jnp.bfloat16):
    entries = jax.random.normal(own_key, shape, jnp.float32) * width
    if len(pieces) > 0:
        entries = block_scale(own_key, shape, pieces, -0.22, 0.18) * entries
    return jnp.clip(entries, min=-most, max=most).astype(held_as)


def heavy_noise(own_key, extent, spread, reach, shards, heavy, kind=jnp.bfloat16):
    drawn = spread * jax.random.normal(own_key, extent, jnp.float32)
    if shards:
        drawn = drawn * block_scale(own_key, extent, shards, -0.22, 0.18)
    return jnp.clip(spiked(drawn, jax.random.fold_in(own_key, 3), *heavy), -reach, reach).astype(kind)


def setup_inputs(seed: int = 0) -> dict:
    streams_of = jax.random.split(jax.random.key(seed), 6)
    return {
        "activations": heavy_noise(streams_of[0], (TOKENS, D), 1.0, 24.0, ((0, 256),), (0, 1, 256, 6.0)),
        "out_grads": centred(streams_of[1], (TOKENS, KV), 1.0, 6.0, ((0, 256),)),
        "master": centred(streams_of[2], (D, KV), 0.02, 0.15, ((0, 256),), jnp.float32),
        "first_moment": centred(streams_of[3], (D, KV), 0.1, 0.6, ((0, 256),), jnp.float32),
        "second_moment": jnp.clip(jnp.exp(math.log(1.0) - 4.6051702 * jax.random.uniform(streams_of[4], (D, KV), jnp.float32) ** block_scale(streams_of[4], (D, KV), ((0, 256),), -0.2, 0.2)), 0.01, 1.0),
    }


def quantize(values):
    blocks = values.reshape(values.shape[:-1] + (KV // BLOCK, BLOCK))
    largest = lax.optimization_barrier(jnp.max(jnp.abs(blocks), axis=-1, keepdims=True))
    scale = (largest + 1e-06) / 127.0
    payload = (blocks / scale).astype(jnp.bfloat16)
    return (payload, scale)

def restore(payload, scale):
    payload = lax.optimization_barrier(payload)
    values = payload.astype(jnp.float32) * scale
    return values.reshape(values.shape[:-2] + (KV,))

def reference(activations, out_grads, master, first_moment, second_moment):

    def node_step(total, node):

        def local_step(summed, local):
            device = node * N_LOCAL + local
            inputs = lax.dynamic_slice_in_dim(activations, device * TOK_DEV, TOK_DEV, 0)
            outputs = lax.dynamic_slice_in_dim(out_grads, device * TOK_DEV, TOK_DEV, 0)
            grad = jnp.dot(inputs.T, outputs, preferred_element_type=jnp.float32)
            return (summed + restore(*quantize(grad)), None)
        first_sum, unused = lax.scan(local_step, jnp.zeros((D, KV), jnp.float32), jnp.arange(N_LOCAL, dtype=jnp.int32))
        return (total + restore(*quantize(first_sum)), None)
    total, unused = lax.scan(node_step, jnp.zeros((D, KV), jnp.float32), jnp.arange(N_NODE, dtype=jnp.int32))
    grad = total / (N_NODE * N_LOCAL)
    new_first = 0.9 * first_moment + 0.1 * grad
    new_second = 0.95 * second_moment + 0.05 * grad * grad
    update = new_first / (1.0 - 0.9 ** 10) / (jnp.sqrt(new_second / (1.0 - 0.95 ** 10)) + 1e-08)
    new_weight = (master - 0.01 * update).astype(jnp.bfloat16)
    return (new_weight, new_first, new_second)
```

```python
import jax
import jax.numpy as jnp
from jax import lax
from jax.experimental import pallas as pl
from jax.experimental.pallas import tpu as pltpu
from jax.sharding import PartitionSpec as P

BLOCK = 256
MESH = pl.DeviceIdType.MESH
F32 = jnp.float32
BF16 = jnp.bfloat16

NX, NZ, NCORE, NYLO, NYHI = 4, 8, 2, 2, 2
NODES, LOCALS = 32, 8
OWN = 16
TOK = 128
COLS = 512
HALVES = COLS // BLOCK
CHUNKS = 4
SLOTS = NODES // CHUNKS
ROWS = SLOTS * OWN
KEEP = ROWS // NCORE


def quantize_restore(values):
    largest = jnp.max(jnp.abs(values), axis=1, keepdims=True)
    scale = (largest + 1e-06) / 127.0
    payload = (values * (1.0 / scale)).astype(BF16)
    return payload.astype(F32) * scale


def kernel(
    act_hbm, grads_hbm, master_hbm, first_hbm, second_hbm,
    weight_out, first_out, second_out,
    act, at_send, at_recv, g, y_send, y_recv, keep, d_send, d_recv, z_send, z_recv, own_sum,
    master, first, second, new_first, new_second, weight,
    load_sem, g_ss, g_rs, a_ss, a_rs, y_ss, y_rs, d_ss, d_rs, z_ss, z_rs, w_ss, w_rs, store_sem,
):
    node = lax.axis_index("node")
    local = lax.axis_index("local")
    core = node % NCORE
    z = (node // NCORE) % NZ
    y_lo = node // (NCORE * NZ)
    x = local % NX
    y_hi = local // NX

    def node_of(yr, dz, cr):
        return (((y_lo + yr) % NYLO) * NZ + (z + dz) % NZ) * NCORE + (core + cr) % NCORE

    def local_of(hr, dx):
        return ((y_hi + hr) % NYHI) * NX + (x + dx) % NX

    def remote(src, dst, ss, rs, to):
        return pltpu.make_async_remote_copy(
            src_ref=src, dst_ref=dst, send_sem=ss, recv_sem=rs, device_id=to, device_id_type=MESH
        )

    local_peers = [(node, local_of(hr, dx)) for hr in range(NYHI) for dx in range(NX) if hr or dx]
    z_peers = [(node_of(yr, dz, 0), local) for dz in range(NZ) for yr in range(NYLO) if dz or yr]
    partner = (node_of(0, 0, 1), local)
    peers = [*local_peers, *z_peers, partner]

    loads = [
        pltpu.make_async_copy(act_hbm, act, load_sem.at[0]),
        *(
            pltpu.make_async_copy(grads_hbm.at[:, pl.ds(b * BLOCK, BLOCK)], g.at[0, b], load_sem.at[1 + b])
            for b in range(HALVES)
        ),
        pltpu.make_async_copy(master_hbm, master, load_sem.at[1 + HALVES]),
        pltpu.make_async_copy(first_hbm, first, load_sem.at[2 + HALVES]),
        pltpu.make_async_copy(second_hbm, second, load_sem.at[3 + HALVES]),
    ]
    for load in loads:
        load.start()
    barrier = pltpu.get_barrier_semaphore()
    for peer in peers:
        pl.semaphore_signal(barrier, inc=1, device_id=peer, device_id_type=MESH)

    loads[0].wait()

    def transpose_chunk(j, carry):
        for cr in range(NCORE):
            for kk in range(2):
                dz = 4 + j if kk == 0 else 3 - j
                for yr in range(NYLO):
                    slot = j * SLOTS + (cr * 2 + kk) * 2 + yr
                    m = node_of(yr, dz, cr)
                    columns = pl.ds(pl.multiple_of(m * (LOCALS * OWN), LOCALS * OWN), LOCALS * OWN)
                    turned = act[:, columns].T
                    for owner in range(LOCALS):
                        dx = (owner % NX - x + NX) % NX
                        hr = (owner // NX - y_hi + NYHI) % NYHI
                        at_send[dx, hr, slot] = turned[owner * OWN : (owner + 1) * OWN]
        return carry

    lax.fori_loop(0, CHUNKS, transpose_chunk, 0)
    for load in loads[1:]:
        load.wait()
    pl.semaphore_wait(barrier, len(peers))

    def g_copy(dx, b):
        return remote(g.at[0, b], g.at[dx, b], g_ss.at[dx - 1, b], g_rs.at[dx - 1, b], (node, local_of(0, dx)))

    def a_copy(dx, hr, j):
        part = pl.ds(j * SLOTS, SLOTS)
        return remote(
            at_send.at[dx, hr, part], at_recv.at[dx - 1, hr, part],
            a_ss.at[dx - 1, hr, j], a_rs.at[dx - 1, hr, j], (node, local_of(0, dx)),
        )

    def y_copy(j, b):
        return remote(y_send.at[j, b], y_recv.at[j, b], y_ss.at[j, b], y_rs.at[j, b], (node, local_of(1, 0)))

    def d_copy(j, b):
        return remote(d_send.at[j, b], d_recv.at[j, b], d_ss.at[j, b], d_rs.at[j, b], partner)

    def z_copy(j, kk, yr):
        dz = 4 + j if kk == 0 else 3 - j
        return remote(
            z_send.at[j, kk, yr], z_recv.at[j, kk, yr],
            z_ss.at[j, kk, yr], z_rs.at[j, kk, yr], (node_of(yr, dz, 0), local),
        )

    def w_copy(i):
        hr, dx = (i + 1) // NX, (i + 1) % NX
        mine = pl.ds(pl.multiple_of(local * OWN, OWN), OWN)
        return remote(weight, weight_out.at[mine], w_ss.at[i], w_rs.at[i], (node, local_of(hr, dx)))

    across = (1, 3, 2)
    for dx in across:
        g_copy(dx, 0).start()
    for j in range(CHUNKS):
        for dx in across:
            a_copy(dx, 1, j).start()
    for dx in across:
        g_copy(dx, 1).start()
    for j in range(CHUNKS):
        for dx in across:
            a_copy(dx, 0, j).start()

    def ring_sum(hr, j, b):
        part = pl.ds(j * SLOTS, SLOTS)
        total = None
        for dx in range(NX):
            inputs = at_send[0, hr, part] if dx == 0 else at_recv[dx - 1, hr, part]
            grad = jnp.dot(inputs.reshape(ROWS, TOK), g[dx, b], preferred_element_type=F32)
            restored = quantize_restore(grad)
            total = restored if total is None else total + restored
        return total

    for b in range(HALVES):
        for dx in across:
            g_copy(dx, b).wait_recv()

        def partner_rows(j, carry, b=b):
            if b == 0:
                for dx in across:
                    a_copy(dx, 1, j).wait_recv()
            y_send[j, b] = ring_sum(1, j, b).astype(BF16)
            y_copy(j, b).start()
            return carry

        lax.fori_loop(0, CHUNKS, partner_rows, 0)

    def to_owners(j):
        for b in range(HALVES):
            d_copy(j, b).wait_recv()
        for kk in range(2):
            for yr in range(NYLO):
                rows = pl.ds((kk * 2 + yr) * OWN, OWN)
                pair = keep[j, :, rows] + d_recv[j, :, rows]
                for b in range(HALVES):
                    z_send[j, kk, yr, :, b * BLOCK : (b + 1) * BLOCK] = pair[b].astype(BF16)
                    if kk == 1 and yr == 0:
                        own_sum[:, b * BLOCK : (b + 1) * BLOCK] = pair[b]
                if kk == 1 and yr == 0:
                    @pl.when(j < CHUNKS - 1)
                    def _():
                        z_copy(j, kk, yr).start()
                else:
                    z_copy(j, kk, yr).start()

    def own_rows(j, carry):
        for dx in across:
            a_copy(dx, 0, j).wait_recv()
        for b in range(HALVES):
            partial = ring_sum(0, j, b)
            y_copy(j, b).wait_recv()
            restored = quantize_restore(partial + y_recv[j, b].astype(F32))
            keep[j, b] = restored[:KEEP]
            d_send[j, b] = restored[KEEP:]
            d_copy(j, b).start()

        @pl.when(j > 0)
        def _():
            to_owners(j - 1)

        return carry

    lax.fori_loop(0, CHUNKS, own_rows, 0)
    to_owners(CHUNKS - 1)

    total = own_sum[...]
    for j in range(CHUNKS):
        for kk in range(2):
            for yr in range(NYLO):
                if (j, kk, yr) != (CHUNKS - 1, 1, 0):
                    z_copy(j, kk, yr).wait_recv()
                    total = total + z_recv[j, kk, yr].astype(F32)
    grad = total / (NODES * LOCALS)
    first_now = 0.9 * first[...] + 0.1 * grad
    second_now = 0.95 * second[...] + 0.05 * grad * grad
    update = first_now / (1.0 - 0.9**10) / (jnp.sqrt(second_now / (1.0 - 0.95**10)) + 1e-08)
    weight[...] = (master[...] - 0.01 * update).astype(BF16)
    new_first[...] = first_now
    new_second[...] = second_now
    for i in range(LOCALS - 1):
        w_copy(i).start()
    mine = pl.ds(pl.multiple_of(local * OWN, OWN), OWN)
    stores = [
        pltpu.make_async_copy(weight, weight_out.at[mine], store_sem.at[0]),
        pltpu.make_async_copy(new_first, first_out, store_sem.at[1]),
        pltpu.make_async_copy(new_second, second_out, store_sem.at[2]),
    ]
    for store in stores:
        store.start()

    for dx in across:
        for b in range(HALVES):
            g_copy(dx, b).wait_send()

    def drain(j, carry):
        for dx in across:
            for hr in range(NYHI):
                a_copy(dx, hr, j).wait_send()
        for b in range(HALVES):
            y_copy(j, b).wait_send()
            d_copy(j, b).wait_send()
        for kk in range(2):
            for yr in range(NYLO):
                if kk == 1 and yr == 0:
                    @pl.when(j < CHUNKS - 1)
                    def _():
                        z_copy(j, kk, yr).wait_send()
                else:
                    z_copy(j, kk, yr).wait_send()
        return carry

    lax.fori_loop(0, CHUNKS, drain, 0)
    for store in stores:
        store.wait()
    for i in range(LOCALS - 1):
        w_copy(i).wait_recv()
    for i in range(LOCALS - 1):
        w_copy(i).wait_send()


def per_device(activations, out_grads, master, first_moment, second_moment):
    anywhere = pl.BlockSpec(memory_space=pl.ANY)
    dma = pltpu.SemaphoreType.DMA
    vmem = pltpu.VMEM
    return pl.pallas_call(
        kernel,
        out_shape=(
            jax.ShapeDtypeStruct((LOCALS * OWN, COLS), BF16),
            jax.ShapeDtypeStruct((OWN, COLS), F32),
            jax.ShapeDtypeStruct((OWN, COLS), F32),
        ),
        in_specs=[anywhere] * 5,
        out_specs=(anywhere,) * 3,
        scratch_shapes=[
            vmem((TOK, NODES * LOCALS * OWN), BF16),
            vmem((NX, NYHI, NODES, OWN, TOK), BF16),
            vmem((NX - 1, NYHI, NODES, OWN, TOK), BF16),
            vmem((NX, HALVES, TOK, BLOCK), BF16),
            vmem((CHUNKS, HALVES, ROWS, BLOCK), BF16),
            vmem((CHUNKS, HALVES, ROWS, BLOCK), BF16),
            vmem((CHUNKS, HALVES, KEEP, BLOCK), F32),
            vmem((CHUNKS, HALVES, KEEP, BLOCK), F32),
            vmem((CHUNKS, HALVES, KEEP, BLOCK), F32),
            vmem((CHUNKS, 2, NYLO, OWN, COLS), BF16),
            vmem((CHUNKS, 2, NYLO, OWN, COLS), BF16),
            vmem((OWN, COLS), F32),
            vmem((OWN, COLS), F32),
            vmem((OWN, COLS), F32),
            vmem((OWN, COLS), F32),
            vmem((OWN, COLS), F32),
            vmem((OWN, COLS), F32),
            vmem((OWN, COLS), BF16),
            dma((4 + HALVES,)),
            dma((NX - 1, HALVES)),
            dma((NX - 1, HALVES)),
            dma((NX - 1, NYHI, CHUNKS)),
            dma((NX - 1, NYHI, CHUNKS)),
            dma((CHUNKS, HALVES)),
            dma((CHUNKS, HALVES)),
            dma((CHUNKS, HALVES)),
            dma((CHUNKS, HALVES)),
            dma((CHUNKS, 2, NYLO)),
            dma((CHUNKS, 2, NYLO)),
            dma((LOCALS - 1,)),
            dma((LOCALS - 1,)),
            dma((3,)),
        ],
        compiler_params=pltpu.CompilerParams(collective_id=0, has_side_effects=True),
    )(activations, out_grads, master, first_moment, second_moment)


def solution(mesh):
    rows = P(("node", "local"), None)
    return jax.shard_map(
        per_device,
        mesh=mesh,
        in_specs=(rows,) * 5,
        out_specs=(P("node", None), rows, rows),
        check_vma=False,
    )
```

```python
import jax
import jax.numpy as jnp
from jax import lax
from jax.experimental import pallas as pl
from jax.experimental.pallas import tpu as pltpu
from jax.sharding import PartitionSpec as P

BLOCK = 256
MESH = pl.DeviceIdType.MESH
F32 = jnp.float32
BF16 = jnp.bfloat16

NX, NY, NZ, NCORE, NYLO, NYHI = 4, 4, 8, 2, 2, 2
NODES, LOCALS = 32, 8
OWN = 16
TOK = 128
COLS = 512
HALVES = COLS // BLOCK
UNITS = 2
FAR = ((4, 3, 5, 2), (6, 1, 7, 0))
QUADS = 4
CLASSES = 4
STEP = (2, 1, 3, 0)
OWN_CLASS = 3
SLOTS = NCORE * QUADS
ROWS = SLOTS * OWN
KEEP = ROWS // NCORE


def quantize_restore(values):
    largest = jnp.max(jnp.abs(values), axis=1, keepdims=True)
    scale = (largest + 1e-06) / 127.0
    payload = (values * (1.0 / scale)).astype(BF16)
    return payload.astype(F32) * scale


def kernel(
    act_hbm, grads_hbm, master_hbm, first_hbm, second_hbm,
    weight_out, first_out, second_out,
    act, at_send, at_recv, g, base, y_send, y_recv, keep, d_send, d_recv, z_send, z_recv, own_sum,
    master, first, second, new_first, new_second, weight,
    load_sem, g_ss, g_rs, a_ss, a_rs, y_ss, y_rs, d_ss, d_rs, z_ss, z_rs, w_ss, w_rs, store_sem,
):
    node = lax.axis_index("node")
    local = lax.axis_index("local")
    core = node % NCORE
    z = (node // NCORE) % NZ
    x = local % NX
    y_hi = local // NX
    y = y_hi * NYLO + node // (NCORE * NZ)

    def device(dx, dy, dz, dc):
        to_y = (y + dy) % NY
        to_node = ((to_y % NYLO) * NZ + (z + dz) % NZ) * NCORE + (core + dc) % NCORE
        return to_node, (to_y // NYLO) * NX + (x + dx) % NX

    def remote(src, dst, ss, rs, to):
        return pltpu.make_async_remote_copy(
            src_ref=src, dst_ref=dst, send_sem=ss, recv_sem=rs, device_id=to, device_id_type=MESH
        )

    peers = [
        *(device(dx, dy, 0, 0) for dy in (0, 2) for dx in range(NX) if dx or dy),
        *(device(0, dy, 0, 0) for dy in (1, 3)),
        *(device(0, 0, dz, 0) for dz in range(1, NZ)),
        device(0, 0, 0, 1),
    ]

    loads = [
        pltpu.make_async_copy(act_hbm, act, load_sem.at[0]),
        *(
            pltpu.make_async_copy(grads_hbm.at[:, pl.ds(b * BLOCK, BLOCK)], g.at[0, b], load_sem.at[1 + b])
            for b in range(HALVES)
        ),
        pltpu.make_async_copy(master_hbm, master, load_sem.at[1 + HALVES]),
        pltpu.make_async_copy(first_hbm, first, load_sem.at[2 + HALVES]),
        pltpu.make_async_copy(second_hbm, second, load_sem.at[3 + HALVES]),
    ]
    for load in loads:
        load.start()
    barrier = pltpu.get_barrier_semaphore()
    for peer in peers:
        pl.semaphore_signal(barrier, inc=1, device_id=peer, device_id_type=MESH)

    loads[0].wait()
    next_hi = ((y + 1) % NY) // NYLO

    def transpose_pair(i, carry):
        yr, cr = i // NCORE, i % NCORE
        for u in range(UNITS):
            for q in range(QUADS):
                m = device(0, yr, FAR[u][q], cr)[0]
                columns = pl.ds(pl.multiple_of(m * (LOCALS * OWN), LOCALS * OWN), LOCALS * OWN)
                turned = act[:, columns].T
                for owner in range(LOCALS):
                    dx = (owner % NX - x + NX) % NX
                    hi = owner // NX
                    kind = (1 - yr) * OWN_CLASS * ((hi + y_hi + 1) % NYHI) + yr * (1 + (hi + next_hi) % NYHI)
                    at_send[dx, kind, u, cr * QUADS + q] = turned[owner * OWN : (owner + 1) * OWN]
        return carry

    lax.fori_loop(0, NYLO * NCORE, transpose_pair, 0)
    for load in loads[1:]:
        load.wait()

    def ring_term(dx, kind, u, b):
        inputs = at_send[0, kind, u] if dx == 0 else at_recv[dx - 1, kind, u]
        grad = jnp.dot(inputs.reshape(ROWS, TOK), g[dx, b], preferred_element_type=F32)
        return quantize_restore(grad)

    def own_terms(kind, carry):
        for u in range(UNITS):
            for b in range(HALVES):
                base[kind, u, b] = ring_term(0, kind, u, b)
        return carry

    lax.fori_loop(0, CLASSES, own_terms, 0)
    pl.semaphore_wait(barrier, len(peers))

    def g_copy(dx, b):
        return remote(g.at[0, b], g.at[dx, b], g_ss.at[dx - 1, b], g_rs.at[dx - 1, b], device(dx, 0, 0, 0))

    def a_copy(dx, kind, u):
        return remote(
            at_send.at[dx, kind, u], at_recv.at[dx - 1, kind, u],
            a_ss.at[dx - 1, kind, u], a_rs.at[dx - 1, kind, u], device(dx, 0, 0, 0),
        )

    def y_copy(kind, step, u, b):
        return remote(
            y_send.at[kind, u, b], y_recv.at[kind, u, b],
            y_ss.at[kind, u, b], y_rs.at[kind, u, b], device(0, step, 0, 0),
        )

    def d_copy(u, b):
        return remote(d_send.at[u, b], d_recv.at[u, b], d_ss.at[u, b], d_rs.at[u, b], device(0, 0, 0, 1))

    def z_copy(u, q):
        return remote(z_send.at[u, q], z_recv.at[u, q], z_ss.at[u, q], z_rs.at[u, q], device(0, 0, FAR[u][q], 0))

    def w_copy(i):
        dy, dx = 2 * ((i + 1) // NX), (i + 1) % NX
        mine = pl.ds(pl.multiple_of(local * OWN, OWN), OWN)
        return remote(weight, weight_out.at[mine], w_ss.at[i], w_rs.at[i], device(dx, dy, 0, 0))

    across = (1, 3, 2)

    def send_inputs(kind, u):
        for dx in across:
            a_copy(dx, kind, u).start()

    for dx in across:
        g_copy(dx, 0).start()
    for u in range(UNITS):
        send_inputs(0, u)
    for dx in across:
        g_copy(dx, 1).start()
    for u in range(UNITS):
        for kind in (1, 2):
            send_inputs(kind, u)
    for u in range(UNITS):
        send_inputs(OWN_CLASS, u)

    def ring_sum(kind, u, b):
        total = base[kind, u, b]
        for dx in range(1, NX):
            total = total + ring_term(dx, kind, u, b)
        return total

    for b in range(HALVES):
        for dx in across:
            g_copy(dx, b).wait_recv()
        for u in range(UNITS):
            if b == 0:
                for dx in across:
                    a_copy(dx, 0, u).wait_recv()
            y_send[0, u, b] = ring_sum(0, u, b).astype(BF16)
            y_copy(0, STEP[0], u, b).start()

    def next_rows(i, carry):
        kind, u = 1 + i % 2, i // 2
        for dx in across:
            a_copy(dx, kind, u).wait_recv()
        for b in range(HALVES):
            y_send[kind, u, b] = ring_sum(kind, u, b).astype(BF16)
            y_copy(kind, 2 * kind - 1, u, b).start()
        return carry

    lax.fori_loop(0, 2 * UNITS, next_rows, 0)

    def own_node(u):
        for dx in across:
            a_copy(dx, OWN_CLASS, u).wait_recv()
        for b in range(HALVES):
            y_copy(0, STEP[0], u, b).wait_recv()
            base[OWN_CLASS, u, b] = quantize_restore(ring_sum(OWN_CLASS, u, b) + y_recv[0, u, b].astype(F32))

    def next_node(u):
        for b in range(HALVES):
            for kind in (1, 2):
                y_copy(kind, STEP[kind], u, b).wait_recv()
            both = quantize_restore(y_recv[1, u, b].astype(F32) + y_recv[2, u, b].astype(F32))
            both = both + base[OWN_CLASS, u, b]
            keep[u, b] = both[:KEEP]
            d_send[u, b] = both[KEEP:]
            d_copy(u, b).start()

    def to_owners(u):
        for b in range(HALVES):
            d_copy(u, b).wait_recv()
        for q in range(QUADS):
            rows = pl.ds(q * OWN, OWN)
            pair = keep[u, :, rows] + d_recv[u, :, rows]
            for b in range(HALVES):
                if FAR[u][q] == 0:
                    own_sum[:, b * BLOCK : (b + 1) * BLOCK] = pair[b]
                else:
                    z_send[u, q, :, b * BLOCK : (b + 1) * BLOCK] = pair[b].astype(BF16)
            if FAR[u][q]:
                z_copy(u, q).start()

    own_node(0)
    next_node(0)
    own_node(1)
    to_owners(0)
    next_node(1)
    to_owners(1)

    total = own_sum[...]
    for u in range(UNITS):
        for q in range(QUADS):
            if FAR[u][q]:
                z_copy(u, q).wait_recv()
                total = total + z_recv[u, q].astype(F32)
    grad = total / (NODES * LOCALS)
    first_now = 0.9 * first[...] + 0.1 * grad
    second_now = 0.95 * second[...] + 0.05 * grad * grad
    update = first_now / (1.0 - 0.9**10) / (jnp.sqrt(second_now / (1.0 - 0.95**10)) + 1e-08)
    weight[...] = (master[...] - 0.01 * update).astype(BF16)
    new_first[...] = first_now
    new_second[...] = second_now
    for i in reversed(range(LOCALS - 1)):
        w_copy(i).start()
    mine = pl.ds(pl.multiple_of(local * OWN, OWN), OWN)
    stores = [
        pltpu.make_async_copy(weight, weight_out.at[mine], store_sem.at[0]),
        pltpu.make_async_copy(new_first, first_out, store_sem.at[1]),
        pltpu.make_async_copy(new_second, second_out, store_sem.at[2]),
    ]
    for store in stores:
        store.start()

    for dx in across:
        for b in range(HALVES):
            g_copy(dx, b).wait_send()

    def drain(u, carry):
        for kind in range(CLASSES):
            for dx in across:
                a_copy(dx, kind, u).wait_send()
        for b in range(HALVES):
            for kind in range(OWN_CLASS):
                y_copy(kind, STEP[kind], u, b).wait_send()
            d_copy(u, b).wait_send()
        return carry

    lax.fori_loop(0, UNITS, drain, 0)
    for u in range(UNITS):
        for q in range(QUADS):
            if FAR[u][q]:
                z_copy(u, q).wait_send()
    for store in stores:
        store.wait()
    for i in range(LOCALS - 1):
        w_copy(i).wait_send()
    for i in range(LOCALS - 1):
        w_copy(i).wait_recv()


def per_device(activations, out_grads, master, first_moment, second_moment):
    anywhere = pl.BlockSpec(memory_space=pl.ANY)
    dma = pltpu.SemaphoreType.DMA
    vmem = pltpu.VMEM
    return pl.pallas_call(
        kernel,
        out_shape=(
            jax.ShapeDtypeStruct((LOCALS * OWN, COLS), BF16),
            jax.ShapeDtypeStruct((OWN, COLS), F32),
            jax.ShapeDtypeStruct((OWN, COLS), F32),
        ),
        in_specs=[anywhere] * 5,
        out_specs=(anywhere,) * 3,
        scratch_shapes=[
            vmem((TOK, NODES * LOCALS * OWN), BF16),
            vmem((NX, CLASSES, UNITS, SLOTS, OWN, TOK), BF16),
            vmem((NX - 1, CLASSES, UNITS, SLOTS, OWN, TOK), BF16),
            vmem((NX, HALVES, TOK, BLOCK), BF16),
            vmem((CLASSES, UNITS, HALVES, ROWS, BLOCK), F32),
            vmem((CLASSES - 1, UNITS, HALVES, ROWS, BLOCK), BF16),
            vmem((CLASSES - 1, UNITS, HALVES, ROWS, BLOCK), BF16),
            vmem((UNITS, HALVES, KEEP, BLOCK), F32),
            vmem((UNITS, HALVES, KEEP, BLOCK), F32),
            vmem((UNITS, HALVES, KEEP, BLOCK), F32),
            vmem((UNITS, QUADS, OWN, COLS), BF16),
            vmem((UNITS, QUADS, OWN, COLS), BF16),
            vmem((OWN, COLS), F32),
            vmem((OWN, COLS), F32),
            vmem((OWN, COLS), F32),
            vmem((OWN, COLS), F32),
            vmem((OWN, COLS), F32),
            vmem((OWN, COLS), F32),
            vmem((OWN, COLS), BF16),
            dma((4 + HALVES,)),
            dma((NX - 1, HALVES)),
            dma((NX - 1, HALVES)),
            dma((NX - 1, CLASSES, UNITS)),
            dma((NX - 1, CLASSES, UNITS)),
            dma((CLASSES - 1, UNITS, HALVES)),
            dma((CLASSES - 1, UNITS, HALVES)),
            dma((UNITS, HALVES)),
            dma((UNITS, HALVES)),
            dma((UNITS, QUADS)),
            dma((UNITS, QUADS)),
            dma((LOCALS - 1,)),
            dma((LOCALS - 1,)),
            dma((3,)),
        ],
        compiler_params=pltpu.CompilerParams(collective_id=0, has_side_effects=True),
    )(activations, out_grads, master, first_moment, second_moment)


def solution(mesh):
    rows = P(("node", "local"), None)
    return jax.shard_map(
        per_device,
        mesh=mesh,
        in_specs=(rows,) * 5,
        out_specs=(P("node", None), rows, rows),
        check_vma=False,
    )
```

```python
import jax
import jax.numpy as jnp
from jax import lax
from jax.experimental import pallas as pl
from jax.experimental.pallas import tpu as pltpu
from jax.sharding import PartitionSpec as P

BLOCK = 256
MESH = pl.DeviceIdType.MESH
F32 = jnp.float32
BF16 = jnp.bfloat16

NX, NY, NZ, NCORE, NYLO, NYHI = 4, 4, 8, 2, 2, 2
NODES, LOCALS = 32, 8
OWN = 16
TOK = 128
COLS = 512
HALVES = COLS // BLOCK
UNITS = 2
FAR = ((4, 3, 5, 2), (6, 1, 7, 0))
QUADS = 4
CLASSES = 4
STEP = (2, 1, 3, 0)
OWN_CLASS = 3
SLOTS = NCORE * QUADS
ROWS = SLOTS * OWN
KEEP = ROWS // NCORE


def quantize_restore(values):
    largest = jnp.max(jnp.abs(values), axis=1, keepdims=True)
    scale = (largest + 1e-06) / 127.0
    payload = (values * (1.0 / scale)).astype(BF16)
    return payload.astype(F32) * scale


def kernel(
    act_hbm, grads_hbm, master_hbm, first_hbm, second_hbm,
    weight_out, first_out, second_out,
    act, at_send, at_recv, g, base, y_send, y_recv, keep, d_send, d_recv, z_send, z_recv, own_sum,
    master, first, second, weight,
    load_sem, g_ss, g_rs, a_ss, a_rs, y_ss, y_rs, d_ss, d_rs, z_ss, z_rs, w_ss, w_rs,
):
    node = lax.axis_index("node")
    local = lax.axis_index("local")
    core = node % NCORE
    z = (node // NCORE) % NZ
    x = local % NX
    y_hi = local // NX
    y = y_hi * NYLO + node // (NCORE * NZ)

    def device(dx, dy, dz, dc):
        to_y = (y + dy) % NY
        to_node = ((to_y % NYLO) * NZ + (z + dz) % NZ) * NCORE + (core + dc) % NCORE
        return to_node, (to_y // NYLO) * NX + (x + dx) % NX

    def remote(src, dst, ss, rs, to):
        return pltpu.make_async_remote_copy(
            src_ref=src, dst_ref=dst, send_sem=ss, recv_sem=rs, device_id=to, device_id_type=MESH
        )

    peers = [
        *(device(dx, dy, 0, 0) for dy in (0, 2) for dx in range(NX) if dx or dy),
        *(device(0, dy, 0, 0) for dy in (1, 3)),
        *(device(0, 0, dz, 0) for dz in range(1, NZ)),
        device(0, 0, 0, 1),
    ]

    loads = [
        pltpu.make_async_copy(act_hbm, act, load_sem.at[0]),
        *(
            pltpu.make_async_copy(grads_hbm.at[:, pl.ds(b * BLOCK, BLOCK)], g.at[0, b], load_sem.at[1 + b])
            for b in range(HALVES)
        ),
        pltpu.make_async_copy(master_hbm, master, load_sem.at[1 + HALVES]),
        pltpu.make_async_copy(first_hbm, first, load_sem.at[2 + HALVES]),
        pltpu.make_async_copy(second_hbm, second, load_sem.at[3 + HALVES]),
    ]
    for load in loads:
        load.start()
    barrier = pltpu.get_barrier_semaphore()
    for peer in peers:
        pl.semaphore_signal(barrier, inc=1, device_id=peer, device_id_type=MESH)

    loads[0].wait()
    next_hi = ((y + 1) % NY) // NYLO

    def transpose_pair(i, carry):
        yr, cr = i // NCORE, i % NCORE
        for u in range(UNITS):
            for q in range(QUADS):
                m = device(0, yr, FAR[u][q], cr)[0]
                columns = pl.ds(pl.multiple_of(m * (LOCALS * OWN), LOCALS * OWN), LOCALS * OWN)
                turned = act[:, columns].T
                for owner in range(LOCALS):
                    dx = (owner % NX - x + NX) % NX
                    hi = owner // NX
                    kind = (1 - yr) * OWN_CLASS * ((hi + y_hi + 1) % NYHI) + yr * (1 + (hi + next_hi) % NYHI)
                    at_send[dx, kind, u, cr * QUADS + q] = turned[owner * OWN : (owner + 1) * OWN]
        return carry

    lax.fori_loop(0, NYLO * NCORE, transpose_pair, 0)
    for load in loads[1:]:
        load.wait()

    def ring_term(dx, kind, u, b):
        inputs = at_send[0, kind, u] if dx == 0 else at_recv[dx - 1, kind, u]
        grad = jnp.dot(inputs.reshape(ROWS, TOK), g[dx, b], preferred_element_type=F32)
        return quantize_restore(grad)

    pl.semaphore_wait(barrier, len(peers))

    def g_copy(dx, b):
        return remote(g.at[0, b], g.at[dx, b], g_ss.at[dx - 1, b], g_rs.at[dx - 1, b], device(dx, 0, 0, 0))

    def a_copy(dx, kind, u):
        return remote(
            at_send.at[dx, kind, u], at_recv.at[dx - 1, kind, u],
            a_ss.at[dx - 1, kind, u], a_rs.at[dx - 1, kind, u], device(dx, 0, 0, 0),
        )

    def y_copy(kind, step, u, b):
        return remote(
            y_send.at[kind, u, b], y_recv.at[kind, u, b],
            y_ss.at[kind, u, b], y_rs.at[kind, u, b], device(0, step, 0, 0),
        )

    def d_copy(u, b):
        return remote(d_send.at[u, b], d_recv.at[u, b], d_ss.at[u, b], d_rs.at[u, b], device(0, 0, 0, 1))

    def z_copy(u, q):
        return remote(z_send.at[u, q], z_recv.at[u, q], z_ss.at[u, q], z_rs.at[u, q], device(0, 0, FAR[u][q], 0))

    def w_copy(i):
        dy, dx = 2 * ((i + 1) // NX), (i + 1) % NX
        mine = pl.ds(pl.multiple_of(local * OWN, OWN), OWN)
        return remote(weight, weight_out.at[mine], w_ss.at[i], w_rs.at[i], device(dx, dy, 0, 0))

    across = (1, 3, 2)

    def send_inputs(kind, u):
        for dx in across:
            a_copy(dx, kind, u).start()

    for dx in across:
        g_copy(dx, 0).start()
    for u in range(UNITS):
        send_inputs(0, u)
    for dx in across:
        g_copy(dx, 1).start()
    for u in range(UNITS):
        for kind in (1, 2):
            send_inputs(kind, u)
    for u in range(UNITS):
        send_inputs(OWN_CLASS, u)

    def own_terms(kind, carry):
        for u in range(UNITS):
            for b in range(HALVES):
                base[kind, u, b] = ring_term(0, kind, u, b)
        return carry

    lax.fori_loop(0, CLASSES, own_terms, 0)

    def ring_sum(kind, u, b):
        total = base[kind, u, b]
        for dx in range(1, NX):
            total = total + ring_term(dx, kind, u, b)
        return total

    for b in range(HALVES):
        for dx in across:
            g_copy(dx, b).wait_recv()
        for u in range(UNITS):
            if b == 0:
                for dx in across:
                    a_copy(dx, 0, u).wait_recv()
            y_send[0, u, b] = ring_sum(0, u, b).astype(BF16)
            y_copy(0, STEP[0], u, b).start()

    def next_rows(i, carry):
        kind, u = 1 + i % 2, i // 2
        for dx in across:
            a_copy(dx, kind, u).wait_recv()
        for b in range(HALVES):
            y_send[kind, u, b] = ring_sum(kind, u, b).astype(BF16)
            y_copy(kind, 2 * kind - 1, u, b).start()
        return carry

    lax.fori_loop(0, 2 * UNITS, next_rows, 0)

    def own_node(u):
        for dx in across:
            a_copy(dx, OWN_CLASS, u).wait_recv()
        for b in range(HALVES):
            y_copy(0, STEP[0], u, b).wait_recv()
            base[OWN_CLASS, u, b] = quantize_restore(ring_sum(OWN_CLASS, u, b) + y_recv[0, u, b].astype(F32))

    def next_node(u):
        for b in range(HALVES):
            for kind in (1, 2):
                y_copy(kind, STEP[kind], u, b).wait_recv()
            both = quantize_restore(y_recv[1, u, b].astype(F32) + y_recv[2, u, b].astype(F32))
            both = both + base[OWN_CLASS, u, b]
            keep[u, b] = both[:KEEP]
            d_send[u, b] = both[KEEP:]
            d_copy(u, b).start()

    def to_owners(u):
        for b in range(HALVES):
            d_copy(u, b).wait_recv()
        for q in range(QUADS):
            rows = pl.ds(q * OWN, OWN)
            pair = keep[u, :, rows] + d_recv[u, :, rows]
            for b in range(HALVES):
                if FAR[u][q] == 0:
                    own_sum[:, b * BLOCK : (b + 1) * BLOCK] = pair[b]
                else:
                    z_send[u, q, :, b * BLOCK : (b + 1) * BLOCK] = pair[b].astype(BF16)
            if FAR[u][q]:
                z_copy(u, q).start()

    own_node(0)
    next_node(0)
    own_node(1)
    to_owners(0)
    next_node(1)
    to_owners(1)

    total = own_sum[...]
    for u in range(UNITS):
        for q in range(QUADS):
            if FAR[u][q]:
                z_copy(u, q).wait_recv()
                total = total + z_recv[u, q].astype(F32)
    grad = total / (NODES * LOCALS)
    first_now = 0.9 * first[...] + 0.1 * grad
    second_now = 0.95 * second[...] + 0.05 * grad * grad
    update = first_now / (1.0 - 0.9**10) / (jnp.sqrt(second_now / (1.0 - 0.95**10)) + 1e-08)
    weight[...] = (master[...] - 0.01 * update).astype(BF16)
    for i in reversed(range(LOCALS - 1)):
        w_copy(i).start()
    weight_out[pl.ds(pl.multiple_of(local * OWN, OWN), OWN)] = weight[...]
    first_out[...] = first_now
    second_out[...] = second_now

    for dx in across:
        for b in range(HALVES):
            g_copy(dx, b).wait_send()

    def drain(u, carry):
        for kind in range(CLASSES):
            for dx in across:
                a_copy(dx, kind, u).wait_send()
        for b in range(HALVES):
            for kind in range(OWN_CLASS):
                y_copy(kind, STEP[kind], u, b).wait_send()
            d_copy(u, b).wait_send()
        return carry

    lax.fori_loop(0, UNITS, drain, 0)
    for u in range(UNITS):
        for q in range(QUADS):
            if FAR[u][q]:
                z_copy(u, q).wait_send()
    for i in range(LOCALS - 1):
        w_copy(i).wait_send()
    for i in range(LOCALS - 1):
        w_copy(i).wait_recv()


def hand_out(weight, first, second, weight_out, first_out, second_out, sem):
    copies = [
        pltpu.make_async_copy(weight, weight_out, sem.at[0]),
        pltpu.make_async_copy(first, first_out, sem.at[1]),
        pltpu.make_async_copy(second, second_out, sem.at[2]),
    ]
    for copy in copies:
        copy.start()
    for copy in copies:
        copy.wait()


def per_device(activations, out_grads, master, first_moment, second_moment):
    anywhere = pl.BlockSpec(memory_space=pl.ANY)
    dma = pltpu.SemaphoreType.DMA
    vmem = pltpu.VMEM
    results = (
        jax.ShapeDtypeStruct((LOCALS * OWN, COLS), BF16),
        jax.ShapeDtypeStruct((OWN, COLS), F32),
        jax.ShapeDtypeStruct((OWN, COLS), F32),
    )
    arguments = (activations, out_grads, master, first_moment, second_moment)
    made = pl.pallas_call(
        kernel,
        out_shape=tuple(vmem(result.shape, result.dtype) for result in results),
        in_specs=[pl.BlockSpec(memory_space=pltpu.HBM)] * 5,
        out_specs=(pl.BlockSpec(memory_space=vmem),) * 3,
        scratch_shapes=[
            vmem((TOK, NODES * LOCALS * OWN), BF16),
            vmem((NX, CLASSES, UNITS, SLOTS, OWN, TOK), BF16),
            vmem((NX - 1, CLASSES, UNITS, SLOTS, OWN, TOK), BF16),
            vmem((NX, HALVES, TOK, BLOCK), BF16),
            vmem((CLASSES, UNITS, HALVES, ROWS, BLOCK), F32),
            vmem((CLASSES - 1, UNITS, HALVES, ROWS, BLOCK), BF16),
            vmem((CLASSES - 1, UNITS, HALVES, ROWS, BLOCK), BF16),
            vmem((UNITS, HALVES, KEEP, BLOCK), F32),
            vmem((UNITS, HALVES, KEEP, BLOCK), F32),
            vmem((UNITS, HALVES, KEEP, BLOCK), F32),
            vmem((UNITS, QUADS, OWN, COLS), BF16),
            vmem((UNITS, QUADS, OWN, COLS), BF16),
            vmem((OWN, COLS), F32),
            vmem((OWN, COLS), F32),
            vmem((OWN, COLS), F32),
            vmem((OWN, COLS), F32),
            vmem((OWN, COLS), BF16),
            dma((4 + HALVES,)),
            dma((NX - 1, HALVES)),
            dma((NX - 1, HALVES)),
            dma((NX - 1, CLASSES, UNITS)),
            dma((NX - 1, CLASSES, UNITS)),
            dma((CLASSES - 1, UNITS, HALVES)),
            dma((CLASSES - 1, UNITS, HALVES)),
            dma((UNITS, HALVES)),
            dma((UNITS, HALVES)),
            dma((UNITS, QUADS)),
            dma((UNITS, QUADS)),
            dma((LOCALS - 1,)),
            dma((LOCALS - 1,)),
        ],
        compiler_params=pltpu.CompilerParams(
            collective_id=0, has_side_effects=True, vmem_limit_bytes=16 * 1024 * 1024
        ),
    )(*(pltpu.with_memory_space_constraint(argument, pltpu.HBM) for argument in arguments))
    return pl.pallas_call(
        hand_out,
        out_shape=results,
        in_specs=[pl.BlockSpec(memory_space=vmem)] * 3,
        out_specs=(anywhere,) * 3,
        scratch_shapes=[dma((3,))],
        compiler_params=pltpu.CompilerParams(vmem_limit_bytes=1024 * 1024),
    )(*made)


def solution(mesh):
    rows = P(("node", "local"), None)
    return jax.shard_map(
        per_device,
        mesh=mesh,
        in_specs=(rows,) * 5,
        out_specs=(P("node", None), rows, rows),
        check_vma=False,
    )
```

```python
import jax
import jax.numpy as jnp
from jax import lax
from jax.experimental import pallas as pl
from jax.experimental.pallas import tpu as pltpu
from jax.sharding import PartitionSpec as P

BLOCK = 256
MESH = pl.DeviceIdType.MESH
F32 = jnp.float32
BF16 = jnp.bfloat16

NX, NY, NZ, NCORE, NYLO, NYHI = 4, 4, 8, 2, 2, 2
NODES, LOCALS = 32, 8
OWN = 16
TOK = 128
COLS = 512
HALVES = COLS // BLOCK
UNITS = 2
FAR = ((4, 3, 5, 2), (6, 1, 7, 0))
QUADS = 4
CLASSES = 4
STEP = (2, 1, 3, 0)
OWN_CLASS = 3
SLOTS = NCORE * QUADS
ROWS = SLOTS * OWN
KEEP = ROWS // NCORE
HOPS = NZ // 2 - 1


def quantize_restore(values):
    largest = jnp.max(jnp.abs(values), axis=1, keepdims=True)
    scale = (largest + 1e-06) / 127.0
    payload = (values * (1.0 / scale)).astype(BF16)
    return payload.astype(F32) * scale


def kernel(
    act_hbm, grads_hbm, master_hbm, first_hbm, second_hbm,
    weight_out, first_out, second_out,
    act, at_send, at_recv, g, base, y_send, y_recv, keep, d_send, d_recv, z_send, z_recv, own_sum,
    master, first, second, weight,
    load_sem, g_ss, g_rs, a_ss, a_rs, y_ss, y_rs, d_ss, d_rs, z_ss, z_rs, w_ss, w_rs, hop_sem,
):
    node = lax.axis_index("node")
    local = lax.axis_index("local")
    core = node % NCORE
    z = (node // NCORE) % NZ
    x = local % NX
    y_hi = local // NX
    y = y_hi * NYLO + node // (NCORE * NZ)

    def device(dx, dy, dz, dc):
        to_y = (y + dy) % NY
        to_node = ((to_y % NYLO) * NZ + (z + dz) % NZ) * NCORE + (core + dc) % NCORE
        return to_node, (to_y // NYLO) * NX + (x + dx) % NX

    def remote(src, dst, ss, rs, to):
        return pltpu.make_async_remote_copy(
            src_ref=src, dst_ref=dst, send_sem=ss, recv_sem=rs, device_id=to, device_id_type=MESH
        )

    beside = [device(0, 0, 1, 0), device(0, 0, NZ - 1, 0)]
    peers = [
        *(device(dx, 0, 0, 0) for dx in range(1, NX)),
        *(device(0, dy, 0, 0) for dy in range(1, NY)),
        *beside,
        device(0, 0, 0, 1),
    ]

    def tell(hop):
        for peer in beside:
            pl.semaphore_signal(hop_sem.at[hop], inc=1, device_id=peer, device_id_type=MESH)

    def heard(hop):
        pl.semaphore_wait(hop_sem.at[hop], len(beside))

    loads = [
        pltpu.make_async_copy(act_hbm, act, load_sem.at[0]),
        *(
            pltpu.make_async_copy(grads_hbm.at[:, pl.ds(b * BLOCK, BLOCK)], g.at[0, b], load_sem.at[1 + b])
            for b in range(HALVES)
        ),
        pltpu.make_async_copy(master_hbm, master, load_sem.at[1 + HALVES]),
        pltpu.make_async_copy(first_hbm, first, load_sem.at[2 + HALVES]),
        pltpu.make_async_copy(second_hbm, second, load_sem.at[3 + HALVES]),
    ]
    for load in loads:
        load.start()
    barrier = pltpu.get_barrier_semaphore()
    for peer in peers:
        pl.semaphore_signal(barrier, inc=1, device_id=peer, device_id_type=MESH)

    loads[0].wait()
    next_hi = ((y + 1) % NY) // NYLO

    def transpose_pair(i, carry):
        yr, cr = i // NCORE, i % NCORE
        for u in range(UNITS):
            for q in range(QUADS):
                m = device(0, yr, FAR[u][q], cr)[0]
                columns = pl.ds(pl.multiple_of(m * (LOCALS * OWN), LOCALS * OWN), LOCALS * OWN)
                turned = act[:, columns].T
                for owner in range(LOCALS):
                    dx = (owner % NX - x + NX) % NX
                    hi = owner // NX
                    kind = (1 - yr) * OWN_CLASS * ((hi + y_hi + 1) % NYHI) + yr * (1 + (hi + next_hi) % NYHI)
                    at_send[dx, kind, u, cr * QUADS + q] = turned[owner * OWN : (owner + 1) * OWN]
        return carry

    lax.fori_loop(0, NYLO * NCORE, transpose_pair, 0)
    for load in loads[1:]:
        load.wait()

    def ring_term(dx, kind, u, b):
        inputs = at_send[0, kind, u] if dx == 0 else at_recv[dx - 1, kind, u]
        grad = jnp.dot(inputs.reshape(ROWS, TOK), g[dx, b], preferred_element_type=F32)
        return quantize_restore(grad)

    pl.semaphore_wait(barrier, len(peers))

    def g_copy(dx, b):
        return remote(g.at[0, b], g.at[dx, b], g_ss.at[dx - 1, b], g_rs.at[dx - 1, b], device(dx, 0, 0, 0))

    def a_copy(dx, kind, u):
        return remote(
            at_send.at[dx, kind, u], at_recv.at[dx - 1, kind, u],
            a_ss.at[dx - 1, kind, u], a_rs.at[dx - 1, kind, u], device(dx, 0, 0, 0),
        )

    def y_copy(kind, step, u, b):
        return remote(
            y_send.at[kind, u, b], y_recv.at[kind, u, b],
            y_ss.at[kind, u, b], y_rs.at[kind, u, b], device(0, step, 0, 0),
        )

    def d_copy(u, b):
        return remote(d_send.at[u, b], d_recv.at[u, b], d_ss.at[u, b], d_rs.at[u, b], device(0, 0, 0, 1))

    def z_copy(u, q):
        return remote(z_send.at[u, q], z_recv.at[u, q], z_ss.at[u, q], z_rs.at[u, q], device(0, 0, FAR[u][q], 0))

    def w_copy(i):
        dy, dx = 2 * ((i + 1) // NX), (i + 1) % NX
        mine = pl.ds(pl.multiple_of(local * OWN, OWN), OWN)
        return remote(weight, weight_out.at[mine], w_ss.at[i], w_rs.at[i], device(dx, dy, 0, 0))

    across = (1, 3, 2)

    def send_inputs(kind, u):
        for dx in across:
            a_copy(dx, kind, u).start()

    for dx in across:
        g_copy(dx, 0).start()
    for u in range(UNITS):
        send_inputs(0, u)
    for dx in across:
        g_copy(dx, 1).start()
    for u in range(UNITS):
        for kind in (1, 2):
            send_inputs(kind, u)
    for u in range(UNITS):
        send_inputs(OWN_CLASS, u)
    tell(0)

    def own_terms(kind, carry):
        for u in range(UNITS):
            for b in range(HALVES):
                base[kind, u, b] = ring_term(0, kind, u, b)
        return carry

    lax.fori_loop(0, CLASSES, own_terms, 0)

    def ring_sum(kind, u, b):
        total = base[kind, u, b]
        for dx in range(1, NX):
            total = total + ring_term(dx, kind, u, b)
        return total

    for b in range(HALVES):
        for dx in across:
            g_copy(dx, b).wait_recv()
        heard(b)
        tell(b + 1)
        for u in range(UNITS):
            if b == 0:
                for dx in across:
                    a_copy(dx, 0, u).wait_recv()
            y_send[0, u, b] = ring_sum(0, u, b).astype(BF16)
            y_copy(0, STEP[0], u, b).start()

    def next_rows(i, carry):
        kind, u = 1 + i % 2, i // 2
        for dx in across:
            a_copy(dx, kind, u).wait_recv()
        for b in range(HALVES):
            y_send[kind, u, b] = ring_sum(kind, u, b).astype(BF16)
            y_copy(kind, 2 * kind - 1, u, b).start()
        return carry

    lax.fori_loop(0, 2 * UNITS, next_rows, 0)
    heard(HOPS - 1)

    def own_node(u):
        for dx in across:
            a_copy(dx, OWN_CLASS, u).wait_recv()
        for b in range(HALVES):
            y_copy(0, STEP[0], u, b).wait_recv()
            base[OWN_CLASS, u, b] = quantize_restore(ring_sum(OWN_CLASS, u, b) + y_recv[0, u, b].astype(F32))

    def next_node(u):
        for b in range(HALVES):
            for kind in (1, 2):
                y_copy(kind, STEP[kind], u, b).wait_recv()
            both = quantize_restore(y_recv[1, u, b].astype(F32) + y_recv[2, u, b].astype(F32))
            both = both + base[OWN_CLASS, u, b]
            keep[u, b] = both[:KEEP]
            d_send[u, b] = both[KEEP:]
            d_copy(u, b).start()

    def to_owners(u):
        for b in range(HALVES):
            d_copy(u, b).wait_recv()
        for q in range(QUADS):
            rows = pl.ds(q * OWN, OWN)
            pair = keep[u, :, rows] + d_recv[u, :, rows]
            for b in range(HALVES):
                if FAR[u][q] == 0:
                    own_sum[:, b * BLOCK : (b + 1) * BLOCK] = pair[b]
                else:
                    z_send[u, q, :, b * BLOCK : (b + 1) * BLOCK] = pair[b].astype(BF16)
            if FAR[u][q]:
                z_copy(u, q).start()

    own_node(0)
    next_node(0)
    own_node(1)
    to_owners(0)
    next_node(1)
    to_owners(1)

    total = own_sum[...]
    for u in range(UNITS):
        for q in range(QUADS):
            if FAR[u][q]:
                z_copy(u, q).wait_recv()
                total = total + z_recv[u, q].astype(F32)
    grad = total / (NODES * LOCALS)
    first_now = 0.9 * first[...] + 0.1 * grad
    second_now = 0.95 * second[...] + 0.05 * grad * grad
    update = first_now / (1.0 - 0.9**10) / (jnp.sqrt(second_now / (1.0 - 0.95**10)) + 1e-08)
    weight[...] = (master[...] - 0.01 * update).astype(BF16)
    for i in (5, 4, 6, 3, 1, 0, 2):
        w_copy(i).start()
    weight_out[pl.ds(pl.multiple_of(local * OWN, OWN), OWN)] = weight[...]
    first_out[...] = first_now
    second_out[...] = second_now

    for dx in across:
        for b in range(HALVES):
            g_copy(dx, b).wait_send()

    def drain(u, carry):
        for kind in range(CLASSES):
            for dx in across:
                a_copy(dx, kind, u).wait_send()
        for b in range(HALVES):
            for kind in range(OWN_CLASS):
                y_copy(kind, STEP[kind], u, b).wait_send()
            d_copy(u, b).wait_send()
        return carry

    lax.fori_loop(0, UNITS, drain, 0)
    for u in range(UNITS):
        for q in range(QUADS):
            if FAR[u][q]:
                z_copy(u, q).wait_send()
    for i in range(LOCALS - 1):
        w_copy(i).wait_send()
    for i in range(LOCALS - 1):
        w_copy(i).wait_recv()


def hand_out(weight, first, second, weight_out, first_out, second_out, sem):
    copies = [
        pltpu.make_async_copy(weight, weight_out, sem.at[0]),
        pltpu.make_async_copy(first, first_out, sem.at[1]),
        pltpu.make_async_copy(second, second_out, sem.at[2]),
    ]
    for copy in copies:
        copy.start()
    for copy in copies:
        copy.wait()


def per_device(activations, out_grads, master, first_moment, second_moment):
    anywhere = pl.BlockSpec(memory_space=pl.ANY)
    dma = pltpu.SemaphoreType.DMA
    vmem = pltpu.VMEM
    results = (
        jax.ShapeDtypeStruct((LOCALS * OWN, COLS), BF16),
        jax.ShapeDtypeStruct((OWN, COLS), F32),
        jax.ShapeDtypeStruct((OWN, COLS), F32),
    )
    arguments = (activations, out_grads, master, first_moment, second_moment)
    made = pl.pallas_call(
        kernel,
        out_shape=tuple(vmem(result.shape, result.dtype) for result in results),
        in_specs=[pl.BlockSpec(memory_space=pltpu.HBM)] * 5,
        out_specs=(pl.BlockSpec(memory_space=vmem),) * 3,
        scratch_shapes=[
            vmem((TOK, NODES * LOCALS * OWN), BF16),
            vmem((NX, CLASSES, UNITS, SLOTS, OWN, TOK), BF16),
            vmem((NX - 1, CLASSES, UNITS, SLOTS, OWN, TOK), BF16),
            vmem((NX, HALVES, TOK, BLOCK), BF16),
            vmem((CLASSES, UNITS, HALVES, ROWS, BLOCK), F32),
            vmem((CLASSES - 1, UNITS, HALVES, ROWS, BLOCK), BF16),
            vmem((CLASSES - 1, UNITS, HALVES, ROWS, BLOCK), BF16),
            vmem((UNITS, HALVES, KEEP, BLOCK), F32),
            vmem((UNITS, HALVES, KEEP, BLOCK), F32),
            vmem((UNITS, HALVES, KEEP, BLOCK), F32),
            vmem((UNITS, QUADS, OWN, COLS), BF16),
            vmem((UNITS, QUADS, OWN, COLS), BF16),
            vmem((OWN, COLS), F32),
            vmem((OWN, COLS), F32),
            vmem((OWN, COLS), F32),
            vmem((OWN, COLS), F32),
            vmem((OWN, COLS), BF16),
            dma((4 + HALVES,)),
            dma((NX - 1, HALVES)),
            dma((NX - 1, HALVES)),
            dma((NX - 1, CLASSES, UNITS)),
            dma((NX - 1, CLASSES, UNITS)),
            dma((CLASSES - 1, UNITS, HALVES)),
            dma((CLASSES - 1, UNITS, HALVES)),
            dma((UNITS, HALVES)),
            dma((UNITS, HALVES)),
            dma((UNITS, QUADS)),
            dma((UNITS, QUADS)),
            dma((LOCALS - 1,)),
            dma((LOCALS - 1,)),
            pltpu.SemaphoreType.REGULAR((HOPS,)),
        ],
        compiler_params=pltpu.CompilerParams(
            collective_id=0, has_side_effects=True, vmem_limit_bytes=16 * 1024 * 1024
        ),
    )(*(pltpu.with_memory_space_constraint(argument, pltpu.HBM) for argument in arguments))
    return pl.pallas_call(
        hand_out,
        out_shape=results,
        in_specs=[pl.BlockSpec(memory_space=vmem)] * 3,
        out_specs=(anywhere,) * 3,
        scratch_shapes=[dma((3,))],
        compiler_params=pltpu.CompilerParams(vmem_limit_bytes=1024 * 1024),
    )(*made)


def solution(mesh):
    rows = P(("node", "local"), None)
    return jax.shard_map(
        per_device,
        mesh=mesh,
        in_specs=(rows,) * 5,
        out_specs=(P("node", None), rows, rows),
        check_vma=False,
    )
```

```python
import jax
import jax.numpy as jnp
from jax import lax
from jax.experimental import pallas as pl
from jax.experimental.pallas import tpu as pltpu
from jax.sharding import PartitionSpec as P

BLOCK = 256
MESH = pl.DeviceIdType.MESH
F32 = jnp.float32
BF16 = jnp.bfloat16

NX, NY, NZ, NCORE, NYLO, NYHI = 4, 4, 8, 2, 2, 2
NODES, LOCALS = 32, 8
OWN = 16
TOK = 128
COLS = 512
HALVES = COLS // BLOCK
UNITS = 4
FAR = ((4, 3), (5, 2), (6, 1), (7, 0))
QUADS = 2
CLASSES = 4
STEP = (2, 1, 3, 0)
OWN_CLASS = 3
BOTH = tuple(range(HALVES))
SLOTS = NCORE * QUADS
ROWS = SLOTS * OWN
KEEP = ROWS // NCORE
HOPS = NZ // 2 - 1


def quantize_restore(values):
    largest = jnp.max(jnp.abs(values), axis=1, keepdims=True)
    scale = (largest + 1e-06) / 127.0
    payload = (values * (1.0 / scale)).astype(BF16)
    return payload.astype(F32) * scale


def kernel(
    act_hbm, grads_hbm, master_hbm, first_hbm, second_hbm,
    weight_out, first_out, second_out,
    act, at_send, at_recv, g, base, y_send, y_recv, keep, d_send, d_recv, z_send, z_recv, own_sum,
    master, first, second, weight,
    load_sem, g_ss, g_rs, a_ss, a_rs, y_ss, y_rs, d_ss, d_rs, z_ss, z_rs, w_ss, w_rs, hop_sem,
):
    node = lax.axis_index("node")
    local = lax.axis_index("local")
    core = node % NCORE
    z = (node // NCORE) % NZ
    x = local % NX
    y_hi = local // NX
    y = y_hi * NYLO + node // (NCORE * NZ)

    def device(dx, dy, dz, dc):
        to_y = (y + dy) % NY
        to_node = ((to_y % NYLO) * NZ + (z + dz) % NZ) * NCORE + (core + dc) % NCORE
        return to_node, (to_y // NYLO) * NX + (x + dx) % NX

    def remote(src, dst, ss, rs, to):
        return pltpu.make_async_remote_copy(
            src_ref=src, dst_ref=dst, send_sem=ss, recv_sem=rs, device_id=to, device_id_type=MESH
        )

    beside = [device(0, 0, 1, 0), device(0, 0, NZ - 1, 0)]
    peers = [
        *(device(dx, 0, 0, 0) for dx in range(1, NX)),
        *(device(0, dy, 0, 0) for dy in range(1, NY)),
        *beside,
        device(0, 0, 0, 1),
    ]

    def tell(hop):
        for peer in beside:
            pl.semaphore_signal(hop_sem.at[hop], inc=1, device_id=peer, device_id_type=MESH)

    def heard(hop):
        pl.semaphore_wait(hop_sem.at[hop], len(beside))

    loads = [
        pltpu.make_async_copy(act_hbm, act, load_sem.at[0]),
        *(
            pltpu.make_async_copy(grads_hbm.at[:, pl.ds(b * BLOCK, BLOCK)], g.at[0, b], load_sem.at[1 + b])
            for b in range(HALVES)
        ),
        pltpu.make_async_copy(master_hbm, master, load_sem.at[1 + HALVES]),
        pltpu.make_async_copy(first_hbm, first, load_sem.at[2 + HALVES]),
        pltpu.make_async_copy(second_hbm, second, load_sem.at[3 + HALVES]),
    ]
    for load in loads:
        load.start()
    barrier = pltpu.get_barrier_semaphore()
    for peer in peers:
        pl.semaphore_signal(barrier, inc=1, device_id=peer, device_id_type=MESH)

    loads[0].wait()
    next_hi = ((y + 1) % NY) // NYLO

    def transpose_pair(i, carry):
        yr, cr = i // NCORE, i % NCORE
        for u in range(UNITS):
            for q in range(QUADS):
                m = device(0, yr, FAR[u][q], cr)[0]
                columns = pl.ds(pl.multiple_of(m * (LOCALS * OWN), LOCALS * OWN), LOCALS * OWN)
                turned = act[:, columns].T
                for owner in range(LOCALS):
                    dx = (owner % NX - x + NX) % NX
                    hi = owner // NX
                    kind = (1 - yr) * OWN_CLASS * ((hi + y_hi + 1) % NYHI) + yr * (1 + (hi + next_hi) % NYHI)
                    at_send[dx, kind, u, cr * QUADS + q] = turned[owner * OWN : (owner + 1) * OWN]
        return carry

    lax.fori_loop(0, NYLO * NCORE, transpose_pair, 0)
    for load in loads[1:]:
        load.wait()

    def ring_term(dx, kind, u, b):
        inputs = at_send[0, kind, u] if dx == 0 else at_recv[dx - 1, kind, u]
        grad = jnp.dot(inputs.reshape(ROWS, TOK), g[dx, b], preferred_element_type=F32)
        return quantize_restore(grad)

    def own_terms(kind, carry):
        for u in range(UNITS):
            for b in range(HALVES):
                base[kind, u, b] = ring_term(0, kind, u, b)
        return carry

    pl.semaphore_wait(barrier, len(peers))

    def g_copy(dx, b):
        return remote(g.at[0, b], g.at[dx, b], g_ss.at[dx - 1, b], g_rs.at[dx - 1, b], device(dx, 0, 0, 0))

    def a_copy(dx, kind, u):
        return remote(
            at_send.at[dx, kind, u], at_recv.at[dx - 1, kind, u],
            a_ss.at[dx - 1, kind, u], a_rs.at[dx - 1, kind, u], device(dx, 0, 0, 0),
        )

    def y_copy(kind, step, u, halves):
        part = pl.ds(halves[0], len(halves))
        sem = u * HALVES + halves[0]
        return remote(
            y_send.at[kind, u, part], y_recv.at[kind, u, part],
            y_ss.at[kind, sem], y_rs.at[kind, sem], device(0, step, 0, 0),
        )

    def d_copy(u):
        return remote(d_send.at[u], d_recv.at[u], d_ss.at[u], d_rs.at[u], device(0, 0, 0, 1))

    def z_copy(u, q):
        return remote(z_send.at[u, q], z_recv.at[u, q], z_ss.at[u, q], z_rs.at[u, q], device(0, 0, FAR[u][q], 0))

    def w_copy(i):
        dy, dx = 2 * ((i + 1) // NX), (i + 1) % NX
        mine = pl.ds(pl.multiple_of(local * OWN, OWN), OWN)
        return remote(weight, weight_out.at[mine], w_ss.at[i], w_rs.at[i], device(dx, dy, 0, 0))

    across = (1, 3, 2)

    def send_inputs(kind, u):
        for dx in across:
            a_copy(dx, kind, u).start()

    for dx in across:
        g_copy(dx, 0).start()
    for u in range(UNITS):
        send_inputs(0, u)
    for dx in across:
        g_copy(dx, 1).start()
    for u in range(UNITS):
        for kind in (1, 2):
            send_inputs(kind, u)
    for u in range(UNITS):
        send_inputs(OWN_CLASS, u)
    tell(0)
    lax.fori_loop(0, CLASSES, own_terms, 0)

    def ring_sum(kind, u, b):
        total = base[kind, u, b]
        for dx in range(1, NX):
            total = total + ring_term(dx, kind, u, b)
        return total

    for b in range(HALVES):
        for dx in across:
            g_copy(dx, b).wait_recv()
        heard(b)
        tell(b + 1)
        for u in range(UNITS):
            if b == 0:
                for dx in across:
                    a_copy(dx, 0, u).wait_recv()
            y_send[0, u, b] = ring_sum(0, u, b).astype(BF16)
            y_copy(0, STEP[0], u, (b,)).start()

    def next_rows(i, carry):
        kind, u = 1 + i % 2, i // 2
        for dx in across:
            a_copy(dx, kind, u).wait_recv()
        sums = [ring_sum(kind, u, b) for b in range(HALVES)]
        for b in range(HALVES):
            y_send[kind, u, b] = sums[b].astype(BF16)
        y_copy(kind, 2 * kind - 1, u, BOTH).start()
        return carry

    lax.fori_loop(0, 2 * UNITS, next_rows, 0)
    heard(HOPS - 1)

    def own_node(u):
        for dx in across:
            a_copy(dx, OWN_CLASS, u).wait_recv()
        for b in range(HALVES):
            y_copy(0, STEP[0], u, (b,)).wait_recv()
        sums = [ring_sum(OWN_CLASS, u, b) + y_recv[0, u, b].astype(F32) for b in range(HALVES)]
        sums = [quantize_restore(total) for total in sums]
        for b in range(HALVES):
            base[OWN_CLASS, u, b] = sums[b]

    def next_node(u):
        for kind in (1, 2):
            y_copy(kind, STEP[kind], u, BOTH).wait_recv()
        for b in range(HALVES):
            both = quantize_restore(y_recv[1, u, b].astype(F32) + y_recv[2, u, b].astype(F32))
            both = both + base[OWN_CLASS, u, b]
            keep[u, b] = both[:KEEP]
            d_send[u, b] = both[KEEP:]
        d_copy(u).start()

    def to_owners(u):
        d_copy(u).wait_recv()
        for q in range(QUADS):
            rows = pl.ds(q * OWN, OWN)
            pair = keep[u, :, rows] + d_recv[u, :, rows]
            for b in range(HALVES):
                if FAR[u][q] == 0:
                    own_sum[:, b * BLOCK : (b + 1) * BLOCK] = pair[b]
                else:
                    z_send[u, q, :, b * BLOCK : (b + 1) * BLOCK] = pair[b].astype(BF16)
            if FAR[u][q]:
                z_copy(u, q).start()

    for u in range(UNITS):
        own_node(u)
        next_node(u)

        @pl.when(core == 0)
        def _(u=u):
            to_owners(u)

    @pl.when(core == 1)
    def _():
        for u in range(UNITS):
            to_owners(u)

    total = own_sum[...]
    for u in range(UNITS):
        for q in range(QUADS):
            if FAR[u][q]:
                z_copy(u, q).wait_recv()
                total = total + z_recv[u, q].astype(F32)
    grad = total / (NODES * LOCALS)
    first_now = 0.9 * first[...] + 0.1 * grad
    second_now = 0.95 * second[...] + 0.05 * grad * grad
    update = first_now / (1.0 - 0.9**10) / (jnp.sqrt(second_now / (1.0 - 0.95**10)) + 1e-08)
    weight[...] = (master[...] - 0.01 * update).astype(BF16)
    for i in (5, 4, 6, 3, 1, 0, 2):
        w_copy(i).start()
    weight_out[pl.ds(pl.multiple_of(local * OWN, OWN), OWN)] = weight[...]
    first_out[...] = first_now
    second_out[...] = second_now

    for dx in across:
        for b in range(HALVES):
            g_copy(dx, b).wait_send()

    def drain(u, carry):
        for kind in range(CLASSES):
            for dx in across:
                a_copy(dx, kind, u).wait_send()
        for b in range(HALVES):
            y_copy(0, STEP[0], u, (b,)).wait_send()
        for kind in (1, 2):
            y_copy(kind, STEP[kind], u, BOTH).wait_send()
        d_copy(u).wait_send()
        return carry

    lax.fori_loop(0, UNITS, drain, 0)
    for u in range(UNITS):
        for q in range(QUADS):
            if FAR[u][q]:
                z_copy(u, q).wait_send()
    for i in range(LOCALS - 1):
        w_copy(i).wait_send()
    for i in range(LOCALS - 1):
        w_copy(i).wait_recv()


def hand_out(weight, first, second, weight_out, first_out, second_out, sem):
    copies = [
        pltpu.make_async_copy(weight, weight_out, sem.at[0]),
        pltpu.make_async_copy(first, first_out, sem.at[1]),
        pltpu.make_async_copy(second, second_out, sem.at[2]),
    ]
    for copy in copies:
        copy.start()
    for copy in copies:
        copy.wait()


def per_device(activations, out_grads, master, first_moment, second_moment):
    anywhere = pl.BlockSpec(memory_space=pl.ANY)
    dma = pltpu.SemaphoreType.DMA
    vmem = pltpu.VMEM
    results = (
        jax.ShapeDtypeStruct((LOCALS * OWN, COLS), BF16),
        jax.ShapeDtypeStruct((OWN, COLS), F32),
        jax.ShapeDtypeStruct((OWN, COLS), F32),
    )
    arguments = (activations, out_grads, master, first_moment, second_moment)
    made = pl.pallas_call(
        kernel,
        out_shape=tuple(vmem(result.shape, result.dtype) for result in results),
        in_specs=[pl.BlockSpec(memory_space=pltpu.HBM)] * 5,
        out_specs=(pl.BlockSpec(memory_space=vmem),) * 3,
        scratch_shapes=[
            vmem((TOK, NODES * LOCALS * OWN), BF16),
            vmem((NX, CLASSES, UNITS, SLOTS, OWN, TOK), BF16),
            vmem((NX - 1, CLASSES, UNITS, SLOTS, OWN, TOK), BF16),
            vmem((NX, HALVES, TOK, BLOCK), BF16),
            vmem((CLASSES, UNITS, HALVES, ROWS, BLOCK), F32),
            vmem((CLASSES - 1, UNITS, HALVES, ROWS, BLOCK), BF16),
            vmem((CLASSES - 1, UNITS, HALVES, ROWS, BLOCK), BF16),
            vmem((UNITS, HALVES, KEEP, BLOCK), F32),
            vmem((UNITS, HALVES, KEEP, BLOCK), F32),
            vmem((UNITS, HALVES, KEEP, BLOCK), F32),
            vmem((UNITS, QUADS, OWN, COLS), BF16),
            vmem((UNITS, QUADS, OWN, COLS), BF16),
            vmem((OWN, COLS), F32),
            vmem((OWN, COLS), F32),
            vmem((OWN, COLS), F32),
            vmem((OWN, COLS), F32),
            vmem((OWN, COLS), BF16),
            dma((4 + HALVES,)),
            dma((NX - 1, HALVES)),
            dma((NX - 1, HALVES)),
            dma((NX - 1, CLASSES, UNITS)),
            dma((NX - 1, CLASSES, UNITS)),
            dma((CLASSES - 1, UNITS * HALVES)),
            dma((CLASSES - 1, UNITS * HALVES)),
            dma((UNITS,)),
            dma((UNITS,)),
            dma((UNITS, QUADS)),
            dma((UNITS, QUADS)),
            dma((LOCALS - 1,)),
            dma((LOCALS - 1,)),
            pltpu.SemaphoreType.REGULAR((HOPS,)),
        ],
        compiler_params=pltpu.CompilerParams(
            collective_id=0, has_side_effects=True, vmem_limit_bytes=16 * 1024 * 1024
        ),
    )(*(pltpu.with_memory_space_constraint(argument, pltpu.HBM) for argument in arguments))
    return pl.pallas_call(
        hand_out,
        out_shape=results,
        in_specs=[pl.BlockSpec(memory_space=vmem)] * 3,
        out_specs=(anywhere,) * 3,
        scratch_shapes=[dma((3,))],
        compiler_params=pltpu.CompilerParams(vmem_limit_bytes=1024 * 1024),
    )(*made)


def solution(mesh):
    rows = P(("node", "local"), None)
    return jax.shard_map(
        per_device,
        mesh=mesh,
        in_specs=(rows,) * 5,
        out_specs=(P("node", None), rows, rows),
        check_vma=False,
    )
```

```python
import jax
import jax.numpy as jnp
from jax import lax
from jax.experimental import pallas as pl
from jax.experimental.pallas import tpu as pltpu
from jax.sharding import PartitionSpec as P

BLOCK = 256
MESH = pl.DeviceIdType.MESH
F32 = jnp.float32
BF16 = jnp.bfloat16

NX, NY, NZ, NCORE, NYLO, NYHI = 4, 4, 8, 2, 2, 2
NODES, LOCALS = 32, 8
OWN = 16
TOK = 128
COLS = 512
HALVES = COLS // BLOCK
UNITS = 4
QUADS = 2
LAST = NZ - 1
CLASSES = 4
STEP = (2, 1, 3, 0)
OWN_CLASS = 3
FIRST = 2
LATER = ((1, 0), (2, 0), (3, 0), (1, 1), (2, 1), (0, 2), (0, 3), (1, 2), (2, 2), (1, 3), (2, 3), (3, 1), (3, 2), (3, 3))
BOTH = tuple(range(HALVES))
SLOTS = NCORE * QUADS
ROWS = SLOTS * OWN
KEEP = ROWS // NCORE
HOPS = NZ // 2 - 1


def quantize_restore(values):
    largest = jnp.max(jnp.abs(values), axis=1, keepdims=True)
    scale = (largest + 1e-06) / 127.0
    payload = (values * (1.0 / scale)).astype(BF16)
    return payload.astype(F32) * scale


def kernel(
    act_hbm, grads_hbm, master_hbm, first_hbm, second_hbm,
    weight_out, first_out, second_out,
    act, at_send, at_recv, g, base, y_send, y_recv, keep, d_send, d_recv, z_send, z_recv, own_sum,
    master, first, second, weight,
    load_sem, g_ss, g_rs, a_ss, a_rs, y_ss, y_rs, d_ss, d_rs, z_ss, z_rs, w_ss, w_rs, hop_sem,
):
    node = lax.axis_index("node")
    local = lax.axis_index("local")
    core = node % NCORE
    z = (node // NCORE) % NZ
    x = local % NX
    y_hi = local // NX
    y = y_hi * NYLO + node // (NCORE * NZ)

    def device(dx, dy, dz, dc):
        to_y = (y + dy) % NY
        to_node = ((to_y % NYLO) * NZ + (z + dz) % NZ) * NCORE + (core + dc) % NCORE
        return to_node, (to_y // NYLO) * NX + (x + dx) % NX

    def away(u, q):
        place = u * QUADS + q
        return 0 if place == LAST else (place + (place + NZ - z) // NZ - z + NZ) % NZ

    def remote(src, dst, ss, rs, to):
        return pltpu.make_async_remote_copy(
            src_ref=src, dst_ref=dst, send_sem=ss, recv_sem=rs, device_id=to, device_id_type=MESH
        )

    beside = [device(0, 0, 1, 0), device(0, 0, NZ - 1, 0)]
    peers = [
        *(device(dx, 0, 0, 0) for dx in (2, 1, 3)),
        *(device(0, dy, 0, 0) for dy in (2, 1, 3)),
        *beside,
        device(0, 0, 0, 1),
    ]

    def tell(hop):
        for peer in beside:
            pl.semaphore_signal(hop_sem.at[hop], inc=1, device_id=peer, device_id_type=MESH)

    def heard(hop):
        pl.semaphore_wait(hop_sem.at[hop], len(beside))

    loads = [
        pltpu.make_async_copy(act_hbm, act, load_sem.at[0]),
        *(
            pltpu.make_async_copy(grads_hbm.at[:, pl.ds(b * BLOCK, BLOCK)], g.at[0, b], load_sem.at[1 + b])
            for b in range(HALVES)
        ),
        pltpu.make_async_copy(master_hbm, master, load_sem.at[1 + HALVES]),
        pltpu.make_async_copy(first_hbm, first, load_sem.at[2 + HALVES]),
        pltpu.make_async_copy(second_hbm, second, load_sem.at[3 + HALVES]),
    ]
    loads[0].start()
    barrier = pltpu.get_barrier_semaphore()
    for peer in peers:
        pl.semaphore_signal(barrier, inc=1, device_id=peer, device_id_type=MESH)
    for load in loads[1:]:
        load.start()

    loads[0].wait()
    next_hi = ((y + 1) % NY) // NYLO

    def transpose_pair(i, carry):
        yr, cr = i // NCORE, i % NCORE
        for u in range(UNITS):
            for q in range(QUADS):
                m = device(0, yr, away(u, q), cr)[0]
                columns = pl.ds(pl.multiple_of(m * (LOCALS * OWN), LOCALS * OWN), LOCALS * OWN)
                turned = act[:, columns].T
                for owner in range(LOCALS):
                    dx = (owner % NX - x + NX) % NX
                    hi = owner // NX
                    kind = (1 - yr) * OWN_CLASS * ((hi + y_hi + 1) % NYHI) + yr * (1 + (hi + next_hi) % NYHI)
                    at_send[dx, kind, u, cr * QUADS + q] = turned[owner * OWN : (owner + 1) * OWN]
        return carry

    lax.fori_loop(0, NYLO * NCORE, transpose_pair, 0)
    for load in loads[1:]:
        load.wait()

    def ring_term(dx, kind, u, b):
        inputs = at_send[0, kind, u] if dx == 0 else at_recv[dx - 1, kind, u]
        grad = jnp.dot(inputs.reshape(ROWS, TOK), g[dx, b], preferred_element_type=F32)
        return quantize_restore(grad)

    def own_terms(kind, carry):
        for u in range(UNITS):
            for b in range(HALVES):
                base[kind, u, b] = ring_term(0, kind, u, b)
        return carry

    pl.semaphore_wait(barrier, len(peers))

    def g_copy(dx, b):
        return remote(g.at[0, b], g.at[dx, b], g_ss.at[dx - 1, b], g_rs.at[dx - 1, b], device(dx, 0, 0, 0))

    def a_copy(dx, kind, u):
        return remote(
            at_send.at[dx, kind, u], at_recv.at[dx - 1, kind, u],
            a_ss.at[dx - 1, kind, u], a_rs.at[dx - 1, kind, u], device(dx, 0, 0, 0),
        )

    def y_copy(kind, step, u, halves):
        part = pl.ds(halves[0], len(halves))
        sem = u * HALVES + halves[0]
        return remote(
            y_send.at[kind, u, part], y_recv.at[kind, u, part],
            y_ss.at[kind, sem], y_rs.at[kind, sem], device(0, step, 0, 0),
        )

    def d_copy(u):
        return remote(d_send.at[u], d_recv.at[u], d_ss.at[u], d_rs.at[u], device(0, 0, 0, 1))

    def z_copy(u, q, dz):
        return remote(z_send.at[u, q], z_recv.at[dz], z_ss.at[u, q], z_rs.at[dz], device(0, 0, dz, 0))

    def w_copy(i):
        dy, dx = 2 * ((i + 1) // NX), (i + 1) % NX
        mine = pl.ds(pl.multiple_of(local * OWN, OWN), OWN)
        return remote(weight, weight_out.at[mine], w_ss.at[i], w_rs.at[i], device(dx, dy, 0, 0))

    across = (1, 3, 2)

    def send_inputs(kind, u):
        for dx in across:
            a_copy(dx, kind, u).start()

    for dx in across:
        g_copy(dx, 0).start()
    for u in range(FIRST):
        send_inputs(0, u)
    for dx in across:
        g_copy(dx, 1).start()
    for kind, u in LATER:
        send_inputs(kind, u)
    tell(0)
    lax.fori_loop(0, CLASSES, own_terms, 0)

    def ring_sum(kind, u, b):
        total = base[kind, u, b]
        for dx in range(1, NX):
            total = total + ring_term(dx, kind, u, b)
        return total

    def first_rows(u, b):
        y_send[0, u, b] = ring_sum(0, u, b).astype(BF16)
        y_copy(0, STEP[0], u, (b,)).start()

    for b in range(HALVES):
        for dx in across:
            g_copy(dx, b).wait_recv()
        heard(b)
        tell(b + 1)
        for u in range(FIRST):
            if b == 0:
                for dx in across:
                    a_copy(dx, 0, u).wait_recv()
            first_rows(u, b)
    def next_rows(i, carry):
        kind, u = 1 + i % 2, i // 2
        for dx in across:
            a_copy(dx, kind, u).wait_recv()
        sums = [ring_sum(kind, u, b) for b in range(HALVES)]
        for b in range(HALVES):
            y_send[kind, u, b] = sums[b].astype(BF16)
        y_copy(kind, 2 * kind - 1, u, BOTH).start()
        return carry

    lax.fori_loop(0, 2 * FIRST, next_rows, 0)
    for u in range(FIRST, UNITS):
        for dx in across:
            a_copy(dx, 0, u).wait_recv()
        for b in range(HALVES):
            first_rows(u, b)
    lax.fori_loop(2 * FIRST, 2 * UNITS - 2, next_rows, 0)
    heard(HOPS - 1)

    def own_node(u):
        for dx in across:
            a_copy(dx, OWN_CLASS, u).wait_recv()
        for b in range(HALVES):
            y_copy(0, STEP[0], u, (b,)).wait_recv()
        sums = [ring_sum(OWN_CLASS, u, b) + y_recv[0, u, b].astype(F32) for b in range(HALVES)]
        sums = [quantize_restore(total) for total in sums]
        for b in range(HALVES):
            base[OWN_CLASS, u, b] = sums[b]

    def next_node(u):
        for kind in (1, 2):
            y_copy(kind, STEP[kind], u, BOTH).wait_recv()
        for b in range(HALVES):
            both = quantize_restore(y_recv[1, u, b].astype(F32) + y_recv[2, u, b].astype(F32))
            both = both + base[OWN_CLASS, u, b]
            keep[u, b] = both[:KEEP]
            d_send[u, b] = both[KEEP:]
        d_copy(u).start()

    def to_owners(u):
        d_copy(u).wait_recv()
        for q in range(QUADS):
            rows = pl.ds(q * OWN, OWN)
            pair = keep[u, :, rows] + d_recv[u, :, rows]
            for b in range(HALVES):
                if u * QUADS + q == LAST:
                    own_sum[:, b * BLOCK : (b + 1) * BLOCK] = pair[b]
                else:
                    z_send[u, q, :, b * BLOCK : (b + 1) * BLOCK] = pair[b].astype(BF16)
            if u * QUADS + q != LAST:
                z_copy(u, q, away(u, q)).start()

    for u in range(UNITS):
        own_node(u)
        next_node(u)

        @pl.when(core == 0)
        def _(u=u):
            to_owners(u)

        if u == 0:
            lax.fori_loop(2 * UNITS - 2, 2 * UNITS, next_rows, 0)
        if u == 2:
            @pl.when(core == 1)
            def _():
                to_owners(0)

    @pl.when(core == 1)
    def _():
        for u in range(1, UNITS):
            to_owners(u)

    total = own_sum[...]
    for dz in range(1, NZ):
        z_copy(0, 0, dz).wait_recv()
        total = total + z_recv[dz].astype(F32)
    grad = total / (NODES * LOCALS)
    first_now = 0.9 * first[...] + 0.1 * grad
    second_now = 0.95 * second[...] + 0.05 * grad * grad
    update = first_now / (1.0 - 0.9**10) / (jnp.sqrt(second_now / (1.0 - 0.95**10)) + 1e-08)
    weight[...] = (master[...] - 0.01 * update).astype(BF16)
    for i in (5, 4, 6, 3, 1, 0, 2):
        w_copy(i).start()
    weight_out[pl.ds(pl.multiple_of(local * OWN, OWN), OWN)] = weight[...]
    first_out[...] = first_now
    second_out[...] = second_now

    for dx in across:
        for b in range(HALVES):
            g_copy(dx, b).wait_send()

    def drain(u, carry):
        for kind in range(CLASSES):
            for dx in across:
                a_copy(dx, kind, u).wait_send()
        for b in range(HALVES):
            y_copy(0, STEP[0], u, (b,)).wait_send()
        for kind in (1, 2):
            y_copy(kind, STEP[kind], u, BOTH).wait_send()
        d_copy(u).wait_send()
        return carry

    lax.fori_loop(0, UNITS, drain, 0)
    for u in range(UNITS):
        for q in range(QUADS):
            if u * QUADS + q != LAST:
                z_copy(u, q, away(u, q)).wait_send()
    for i in range(LOCALS - 1):
        w_copy(i).wait_send()
    for i in range(LOCALS - 1):
        w_copy(i).wait_recv()


def hand_out(weight, first, second, weight_out, first_out, second_out, sem):
    copies = [
        pltpu.make_async_copy(weight, weight_out, sem.at[0]),
        pltpu.make_async_copy(first, first_out, sem.at[1]),
        pltpu.make_async_copy(second, second_out, sem.at[2]),
    ]
    for copy in copies:
        copy.start()
    for copy in copies:
        copy.wait()


def per_device(activations, out_grads, master, first_moment, second_moment):
    anywhere = pl.BlockSpec(memory_space=pl.ANY)
    dma = pltpu.SemaphoreType.DMA
    vmem = pltpu.VMEM
    results = (
        jax.ShapeDtypeStruct((LOCALS * OWN, COLS), BF16),
        jax.ShapeDtypeStruct((OWN, COLS), F32),
        jax.ShapeDtypeStruct((OWN, COLS), F32),
    )
    arguments = (activations, out_grads, master, first_moment, second_moment)
    made = pl.pallas_call(
        kernel,
        out_shape=tuple(vmem(result.shape, result.dtype) for result in results),
        in_specs=[pl.BlockSpec(memory_space=pltpu.HBM)] * 5,
        out_specs=(pl.BlockSpec(memory_space=vmem),) * 3,
        scratch_shapes=[
            vmem((TOK, NODES * LOCALS * OWN), BF16),
            vmem((NX, CLASSES, UNITS, SLOTS, OWN, TOK), BF16),
            vmem((NX - 1, CLASSES, UNITS, SLOTS, OWN, TOK), BF16),
            vmem((NX, HALVES, TOK, BLOCK), BF16),
            vmem((CLASSES, UNITS, HALVES, ROWS, BLOCK), F32),
            vmem((CLASSES - 1, UNITS, HALVES, ROWS, BLOCK), BF16),
            vmem((CLASSES - 1, UNITS, HALVES, ROWS, BLOCK), BF16),
            vmem((UNITS, HALVES, KEEP, BLOCK), F32),
            vmem((UNITS, HALVES, KEEP, BLOCK), F32),
            vmem((UNITS, HALVES, KEEP, BLOCK), F32),
            vmem((UNITS, QUADS, OWN, COLS), BF16),
            vmem((NZ, OWN, COLS), BF16),
            vmem((OWN, COLS), F32),
            vmem((OWN, COLS), F32),
            vmem((OWN, COLS), F32),
            vmem((OWN, COLS), F32),
            vmem((OWN, COLS), BF16),
            dma((4 + HALVES,)),
            dma((NX - 1, HALVES)),
            dma((NX - 1, HALVES)),
            dma((NX - 1, CLASSES, UNITS)),
            dma((NX - 1, CLASSES, UNITS)),
            dma((CLASSES - 1, UNITS * HALVES)),
            dma((CLASSES - 1, UNITS * HALVES)),
            dma((UNITS,)),
            dma((UNITS,)),
            dma((UNITS, QUADS)),
            dma((NZ,)),
            dma((LOCALS - 1,)),
            dma((LOCALS - 1,)),
            pltpu.SemaphoreType.REGULAR((HOPS,)),
        ],
        compiler_params=pltpu.CompilerParams(
            collective_id=0, has_side_effects=True, vmem_limit_bytes=16 * 1024 * 1024
        ),
    )(*(pltpu.with_memory_space_constraint(argument, pltpu.HBM) for argument in arguments))
    return pl.pallas_call(
        hand_out,
        out_shape=results,
        in_specs=[pl.BlockSpec(memory_space=vmem)] * 3,
        out_specs=(anywhere,) * 3,
        scratch_shapes=[dma((3,))],
        compiler_params=pltpu.CompilerParams(vmem_limit_bytes=1024 * 1024),
    )(*made)


def solution(mesh):
    rows = P(("node", "local"), None)
    return jax.shard_map(
        per_device,
        mesh=mesh,
        in_specs=(rows,) * 5,
        out_specs=(P("node", None), rows, rows),
        check_vma=False,
    )
```

```python
import jax
import jax.numpy as jnp
from jax import lax
from jax.experimental import pallas as pl
from jax.experimental.pallas import tpu as pltpu
from jax.sharding import PartitionSpec as P

BLOCK = 256
MESH = pl.DeviceIdType.MESH
F32 = jnp.float32
BF16 = jnp.bfloat16

NX, NY, NZ, NCORE, NYLO, NYHI = 4, 4, 8, 2, 2, 2
NODES, LOCALS = 32, 8
OWN = 16
TOK = 128
COLS = 512
HALVES = COLS // BLOCK
UNITS = 4
QUADS = 2
LAST = NZ - 1
CLASSES = 4
STEP = (2, 1, 3, 0)
OWN_CLASS = 3
FIRST = 2
LATER = ((1, 0), (2, 0), (3, 0), (1, 1), (2, 1), (0, 2), (0, 3), (1, 2), (2, 2), (1, 3), (2, 3), (3, 1), (3, 2), (3, 3))
BOTH = tuple(range(HALVES))
SLOTS = NCORE * QUADS
ROWS = SLOTS * OWN
KEEP = ROWS // NCORE
REACH = (1, 2, 4)


def quantize_restore(values):
    largest = jnp.max(jnp.abs(values), axis=1, keepdims=True)
    scale = (largest + 1e-06) / 127.0
    payload = (values * (1.0 / scale)).astype(BF16)
    return payload.astype(F32) * scale


def kernel(
    act_hbm, grads_hbm, master_hbm, first_hbm, second_hbm,
    weight_out, first_out, second_out,
    act, at_send, at_recv, g, base, y_send, y_recv, keep, d_send, d_recv, z_send, z_recv, own_sum,
    master, first, second, weight,
    load_sem, g_ss, g_rs, a_ss, a_rs, y_ss, y_rs, d_ss, d_rs, z_ss, z_rs, w_ss, w_rs, hop_sem,
):
    node = lax.axis_index("node")
    local = lax.axis_index("local")
    core = node % NCORE
    z = (node // NCORE) % NZ
    x = local % NX
    y_hi = local // NX
    y = y_hi * NYLO + node // (NCORE * NZ)

    def device(dx, dy, dz, dc):
        to_y = (y + dy) % NY
        to_node = ((to_y % NYLO) * NZ + (z + dz) % NZ) * NCORE + (core + dc) % NCORE
        return to_node, (to_y // NYLO) * NX + (x + dx) % NX

    def away(u, q):
        place = u * QUADS + q
        return 0 if place == LAST else (place + (place + NZ - z) // NZ - z + NZ) % NZ

    def remote(src, dst, ss, rs, to):
        return pltpu.make_async_remote_copy(
            src_ref=src, dst_ref=dst, send_sem=ss, recv_sem=rs, device_id=to, device_id_type=MESH
        )

    peers = [
        *(device(dx, 0, 0, 0) for dx in range(1, NX)),
        *(device(0, dy, 0, 0) for dy in range(1, NY)),
        device(0, 0, 0, 1),
    ]
    def along(d):
        return (z + NZ - d) // NZ + 1 - (z + d) // NZ

    def signal_along(sem, d):
        @pl.when(z < NZ - d)
        def _():
            pl.semaphore_signal(sem, inc=1, device_id=device(0, 0, d, 0), device_id_type=MESH)

        @pl.when(z >= d)
        def _():
            pl.semaphore_signal(sem, inc=1, device_id=device(0, 0, NZ - d, 0), device_id_type=MESH)

    def tell(hop):
        signal_along(hop_sem.at[hop], REACH[hop])

    def heard(hop):
        pl.semaphore_wait(hop_sem.at[hop], along(REACH[hop]))

    loads = [
        pltpu.make_async_copy(act_hbm, act, load_sem.at[0]),
        *(
            pltpu.make_async_copy(grads_hbm.at[:, pl.ds(b * BLOCK, BLOCK)], g.at[0, b], load_sem.at[1 + b])
            for b in range(HALVES)
        ),
        pltpu.make_async_copy(master_hbm, master, load_sem.at[1 + HALVES]),
        pltpu.make_async_copy(first_hbm, first, load_sem.at[2 + HALVES]),
        pltpu.make_async_copy(second_hbm, second, load_sem.at[3 + HALVES]),
    ]
    loads[0].start()
    barrier = pltpu.get_barrier_semaphore()
    for peer in peers:
        pl.semaphore_signal(barrier, inc=1, device_id=peer, device_id_type=MESH)
    signal_along(barrier, 1)
    for load in loads[1:]:
        load.start()

    loads[0].wait()
    next_hi = ((y + 1) % NY) // NYLO

    def transpose_pair(i, carry):
        yr, cr = i // NCORE, i % NCORE
        for u in range(UNITS):
            for q in range(QUADS):
                m = device(0, yr, away(u, q), cr)[0]
                columns = pl.ds(pl.multiple_of(m * (LOCALS * OWN), LOCALS * OWN), LOCALS * OWN)
                turned = act[:, columns].T
                for owner in range(LOCALS):
                    dx = (owner % NX - x + NX) % NX
                    hi = owner // NX
                    kind = (1 - yr) * OWN_CLASS * ((hi + y_hi + 1) % NYHI) + yr * (1 + (hi + next_hi) % NYHI)
                    at_send[dx, kind, u, cr * QUADS + q] = turned[owner * OWN : (owner + 1) * OWN]
        return carry

    lax.fori_loop(0, NYLO * NCORE, transpose_pair, 0)
    for load in loads[1:]:
        load.wait()

    def ring_term(dx, kind, u, b):
        inputs = at_send[0, kind, u] if dx == 0 else at_recv[dx - 1, kind, u]
        grad = jnp.dot(inputs.reshape(ROWS, TOK), g[dx, b], preferred_element_type=F32)
        return quantize_restore(grad)

    def own_terms(kind, carry):
        for u in range(UNITS):
            for b in range(HALVES):
                base[kind, u, b] = ring_term(0, kind, u, b)
        return carry

    pl.semaphore_wait(barrier, len(peers) + along(1))

    def g_copy(dx, b):
        return remote(g.at[0, b], g.at[dx, b], g_ss.at[dx - 1, b], g_rs.at[dx - 1, b], device(dx, 0, 0, 0))

    def a_copy(dx, kind, u):
        return remote(
            at_send.at[dx, kind, u], at_recv.at[dx - 1, kind, u],
            a_ss.at[dx - 1, kind, u], a_rs.at[dx - 1, kind, u], device(dx, 0, 0, 0),
        )

    def y_copy(kind, step, u, halves):
        part = pl.ds(halves[0], len(halves))
        sem = u * HALVES + halves[0]
        return remote(
            y_send.at[kind, u, part], y_recv.at[kind, u, part],
            y_ss.at[kind, sem], y_rs.at[kind, sem], device(0, step, 0, 0),
        )

    def d_copy(u):
        return remote(d_send.at[u], d_recv.at[u], d_ss.at[u], d_rs.at[u], device(0, 0, 0, 1))

    def z_copy(u, q, dz):
        return remote(z_send.at[u, q], z_recv.at[dz], z_ss.at[u, q], z_rs.at[dz], device(0, 0, dz, 0))

    def w_copy(i):
        dy, dx = 2 * ((i + 1) // NX), (i + 1) % NX
        mine = pl.ds(pl.multiple_of(local * OWN, OWN), OWN)
        return remote(weight, weight_out.at[mine], w_ss.at[i], w_rs.at[i], device(dx, dy, 0, 0))

    across = (1, 3, 2)

    def send_inputs(kind, u):
        for dx in across:
            a_copy(dx, kind, u).start()

    for dx in across:
        g_copy(dx, 0).start()
    for u in range(FIRST):
        send_inputs(0, u)
    for dx in across:
        g_copy(dx, 1).start()
    for kind, u in LATER:
        send_inputs(kind, u)
    tell(0)
    lax.fori_loop(0, CLASSES, own_terms, 0)

    def ring_sum(kind, u, b):
        total = base[kind, u, b]
        for dx in range(1, NX):
            total = total + ring_term(dx, kind, u, b)
        return total

    def first_rows(u, b):
        y_send[0, u, b] = ring_sum(0, u, b).astype(BF16)
        y_copy(0, STEP[0], u, (b,)).start()

    for b in range(HALVES):
        for dx in across:
            g_copy(dx, b).wait_recv()
        heard(b)
        tell(b + 1)
        for u in range(FIRST):
            if b == 0:
                for dx in across:
                    a_copy(dx, 0, u).wait_recv()
            first_rows(u, b)
    def next_rows(i, carry):
        kind, u = 1 + i % 2, i // 2
        for dx in across:
            a_copy(dx, kind, u).wait_recv()
        sums = [ring_sum(kind, u, b) for b in range(HALVES)]
        for b in range(HALVES):
            y_send[kind, u, b] = sums[b].astype(BF16)
        y_copy(kind, 2 * kind - 1, u, BOTH).start()
        return carry

    lax.fori_loop(0, 2 * FIRST, next_rows, 0)
    for u in range(FIRST, UNITS):
        for dx in across:
            a_copy(dx, 0, u).wait_recv()
        for b in range(HALVES):
            first_rows(u, b)

    def own_node(u):
        for dx in across:
            a_copy(dx, OWN_CLASS, u).wait_recv()
        for b in range(HALVES):
            y_copy(0, STEP[0], u, (b,)).wait_recv()
        sums = [ring_sum(OWN_CLASS, u, b) + y_recv[0, u, b].astype(F32) for b in range(HALVES)]
        sums = [quantize_restore(total) for total in sums]
        for b in range(HALVES):
            base[OWN_CLASS, u, b] = sums[b]

    def next_node(u):
        for kind in (1, 2):
            y_copy(kind, STEP[kind], u, BOTH).wait_recv()
        for b in range(HALVES):
            both = quantize_restore(y_recv[1, u, b].astype(F32) + y_recv[2, u, b].astype(F32))
            both = both + base[OWN_CLASS, u, b]
            keep[u, b] = both[:KEEP]
            d_send[u, b] = both[KEEP:]
        d_copy(u).start()

    def to_owners(u):
        d_copy(u).wait_recv()
        for q in range(QUADS):
            rows = pl.ds(q * OWN, OWN)
            pair = keep[u, :, rows] + d_recv[u, :, rows]
            for b in range(HALVES):
                if u * QUADS + q == LAST:
                    own_sum[:, b * BLOCK : (b + 1) * BLOCK] = pair[b]
                else:
                    z_send[u, q, :, b * BLOCK : (b + 1) * BLOCK] = pair[b].astype(BF16)
            if u * QUADS + q != LAST:
                z_copy(u, q, away(u, q)).start()

    for u in range(UNITS):
        own_node(u)
        if u >= 2:
            @pl.when(core == 1)
            def _(u=u):
                to_owners(u - 2)

        next_node(u)
        if u == 0:
            heard(2)

        @pl.when(core == 0)
        def _(u=u):
            to_owners(u)

        if u == 0:
            lax.fori_loop(2 * FIRST, 2 * UNITS, next_rows, 0)

    @pl.when(core == 1)
    def _():
        for u in range(2, UNITS):
            to_owners(u)

    total = own_sum[...]
    for dz in range(1, NZ):
        z_copy(0, 0, dz).wait_recv()
        total = total + z_recv[dz].astype(F32)
    grad = total / (NODES * LOCALS)
    first_now = 0.9 * first[...] + 0.1 * grad
    second_now = 0.95 * second[...] + 0.05 * grad * grad
    update = first_now / (1.0 - 0.9**10) / (jnp.sqrt(second_now / (1.0 - 0.95**10)) + 1e-08)
    weight[...] = (master[...] - 0.01 * update).astype(BF16)
    for i in (5, 4, 6, 3, 1, 0, 2):
        w_copy(i).start()
    weight_out[pl.ds(pl.multiple_of(local * OWN, OWN), OWN)] = weight[...]
    first_out[...] = first_now
    second_out[...] = second_now

    for dx in across:
        for b in range(HALVES):
            g_copy(dx, b).wait_send()

    def drain(u, carry):
        for kind in range(CLASSES):
            for dx in across:
                a_copy(dx, kind, u).wait_send()
        for b in range(HALVES):
            y_copy(0, STEP[0], u, (b,)).wait_send()
        for kind in (1, 2):
            y_copy(kind, STEP[kind], u, BOTH).wait_send()
        d_copy(u).wait_send()
        return carry

    lax.fori_loop(0, UNITS, drain, 0)
    for u in range(UNITS):
        for q in range(QUADS):
            if u * QUADS + q != LAST:
                z_copy(u, q, away(u, q)).wait_send()
    for i in range(LOCALS - 1):
        w_copy(i).wait_send()
    for i in range(LOCALS - 1):
        w_copy(i).wait_recv()


def hand_out(weight, first, second, weight_out, first_out, second_out, sem):
    copies = [
        pltpu.make_async_copy(weight, weight_out, sem.at[0]),
        pltpu.make_async_copy(first, first_out, sem.at[1]),
        pltpu.make_async_copy(second, second_out, sem.at[2]),
    ]
    for copy in copies:
        copy.start()
    for copy in copies:
        copy.wait()


def per_device(activations, out_grads, master, first_moment, second_moment):
    anywhere = pl.BlockSpec(memory_space=pl.ANY)
    dma = pltpu.SemaphoreType.DMA
    vmem = pltpu.VMEM
    results = (
        jax.ShapeDtypeStruct((LOCALS * OWN, COLS), BF16),
        jax.ShapeDtypeStruct((OWN, COLS), F32),
        jax.ShapeDtypeStruct((OWN, COLS), F32),
    )
    arguments = (activations, out_grads, master, first_moment, second_moment)
    made = pl.pallas_call(
        kernel,
        out_shape=tuple(vmem(result.shape, result.dtype) for result in results),
        in_specs=[pl.BlockSpec(memory_space=pltpu.HBM)] * 5,
        out_specs=(pl.BlockSpec(memory_space=vmem),) * 3,
        scratch_shapes=[
            vmem((TOK, NODES * LOCALS * OWN), BF16),
            vmem((NX, CLASSES, UNITS, SLOTS, OWN, TOK), BF16),
            vmem((NX - 1, CLASSES, UNITS, SLOTS, OWN, TOK), BF16),
            vmem((NX, HALVES, TOK, BLOCK), BF16),
            vmem((CLASSES, UNITS, HALVES, ROWS, BLOCK), F32),
            vmem((CLASSES - 1, UNITS, HALVES, ROWS, BLOCK), BF16),
            vmem((CLASSES - 1, UNITS, HALVES, ROWS, BLOCK), BF16),
            vmem((UNITS, HALVES, KEEP, BLOCK), F32),
            vmem((UNITS, HALVES, KEEP, BLOCK), F32),
            vmem((UNITS, HALVES, KEEP, BLOCK), F32),
            vmem((UNITS, QUADS, OWN, COLS), BF16),
            vmem((NZ, OWN, COLS), BF16),
            vmem((OWN, COLS), F32),
            vmem((OWN, COLS), F32),
            vmem((OWN, COLS), F32),
            vmem((OWN, COLS), F32),
            vmem((OWN, COLS), BF16),
            dma((4 + HALVES,)),
            dma((NX - 1, HALVES)),
            dma((NX - 1, HALVES)),
            dma((NX - 1, CLASSES, UNITS)),
            dma((NX - 1, CLASSES, UNITS)),
            dma((CLASSES - 1, UNITS * HALVES)),
            dma((CLASSES - 1, UNITS * HALVES)),
            dma((UNITS,)),
            dma((UNITS,)),
            dma((UNITS, QUADS)),
            dma((NZ,)),
            dma((LOCALS - 1,)),
            dma((LOCALS - 1,)),
            pltpu.SemaphoreType.REGULAR((len(REACH),)),
        ],
        compiler_params=pltpu.CompilerParams(
            collective_id=0, has_side_effects=True, vmem_limit_bytes=16 * 1024 * 1024
        ),
    )(*(pltpu.with_memory_space_constraint(argument, pltpu.HBM) for argument in arguments))
    return pl.pallas_call(
        hand_out,
        out_shape=results,
        in_specs=[pl.BlockSpec(memory_space=vmem)] * 3,
        out_specs=(anywhere,) * 3,
        scratch_shapes=[dma((3,))],
        compiler_params=pltpu.CompilerParams(vmem_limit_bytes=1024 * 1024),
    )(*made)


def solution(mesh):
    rows = P(("node", "local"), None)
    return jax.shard_map(
        per_device,
        mesh=mesh,
        in_specs=(rows,) * 5,
        out_specs=(P("node", None), rows, rows),
        check_vma=False,
    )
```

```python
import jax
import jax.numpy as jnp
from jax import lax
from jax.experimental import pallas as pl
from jax.experimental.pallas import tpu as pltpu
from jax.sharding import PartitionSpec as P

BLOCK = 256
MESH = pl.DeviceIdType.MESH
F32 = jnp.float32
BF16 = jnp.bfloat16

NX, NY, NZ, NCORE, NYLO, NYHI = 4, 4, 8, 2, 2, 2
NODES, LOCALS = 32, 8
OWN = 16
TOK = 128
COLS = 512
HALVES = COLS // BLOCK
UNITS = 4
QUADS = 2
LAST = NZ - 1
CLASSES = 4
STEP = (2, 1, 3, 0)
OWN_CLASS = 3
FIRST = 2
LATER = ((1, 0), (2, 0), (3, 0), (1, 1), (2, 1), (0, 2), (0, 3), (1, 2), (2, 2), (1, 3), (2, 3), (3, 1), (3, 2), (3, 3))
BOTH = tuple(range(HALVES))
SLOTS = NCORE * QUADS
ROWS = SLOTS * OWN
KEEP = ROWS // NCORE
REACH = (1, 2, 4)


def quantize_restore(values):
    largest = jnp.max(jnp.abs(values), axis=1, keepdims=True)
    scale = (largest + 1e-06) / 127.0
    payload = (values * (1.0 / scale)).astype(BF16)
    return payload.astype(F32) * scale


def kernel(
    act_hbm, grads_hbm, master_hbm, first_hbm, second_hbm,
    weight_out, first_out, second_out,
    act, at_send, at_recv, g, base, y_send, y_recv, keep, d_send, d_recv, z_send, z_recv, own_sum,
    master, first, second, weight,
    load_sem, g_ss, g_rs, a_ss, a_rs, y_ss, y_rs, d_ss, d_rs, z_ss, z_rs, w_ss, w_rs, hop_sem,
):
    node = lax.axis_index("node")
    local = lax.axis_index("local")
    core = node % NCORE
    z = (node // NCORE) % NZ
    x = local % NX
    y_hi = local // NX
    y = y_hi * NYLO + node // (NCORE * NZ)

    def device(dx, dy, dz, dc):
        to_y = (y + dy) % NY
        to_node = ((to_y % NYLO) * NZ + (z + dz) % NZ) * NCORE + (core + dc) % NCORE
        return to_node, (to_y // NYLO) * NX + (x + dx) % NX

    def away(u, q):
        place = u * QUADS + q
        return 0 if place == LAST else (place + (place + NZ - z) // NZ - z + NZ) % NZ

    def remote(src, dst, ss, rs, to):
        return pltpu.make_async_remote_copy(
            src_ref=src, dst_ref=dst, send_sem=ss, recv_sem=rs, device_id=to, device_id_type=MESH
        )

    peers = [
        *(device(dx, 0, 0, 0) for dx in range(1, NX)),
        *(device(0, dy, 0, 0) for dy in range(1, NY)),
        device(0, 0, 0, 1),
    ]
    def along(d):
        return (z + NZ - d) // NZ + 1 - (z + d) // NZ

    def signal_along(sem, d):
        @pl.when(z < NZ - d)
        def _():
            pl.semaphore_signal(sem, inc=1, device_id=device(0, 0, d, 0), device_id_type=MESH)

        @pl.when(z >= d)
        def _():
            pl.semaphore_signal(sem, inc=1, device_id=device(0, 0, NZ - d, 0), device_id_type=MESH)

    def tell(hop):
        signal_along(hop_sem.at[hop], REACH[hop])

    def heard(hop):
        pl.semaphore_wait(hop_sem.at[hop], along(REACH[hop]))

    loads = [
        pltpu.make_async_copy(act_hbm, act, load_sem.at[0]),
        *(
            pltpu.make_async_copy(grads_hbm.at[:, pl.ds(b * BLOCK, BLOCK)], g.at[0, b], load_sem.at[1 + b])
            for b in range(HALVES)
        ),
        pltpu.make_async_copy(master_hbm, master, load_sem.at[1 + HALVES]),
        pltpu.make_async_copy(first_hbm, first, load_sem.at[2 + HALVES]),
        pltpu.make_async_copy(second_hbm, second, load_sem.at[3 + HALVES]),
    ]
    loads[0].start()
    barrier = pltpu.get_barrier_semaphore()
    for peer in peers:
        pl.semaphore_signal(barrier, inc=1, device_id=peer, device_id_type=MESH)
    signal_along(barrier, 1)
    for load in loads[1:]:
        load.start()

    loads[0].wait()
    next_hi = ((y + 1) % NY) // NYLO

    def transpose_pair(i, carry):
        yr, cr = i // NCORE, i % NCORE
        for u in range(UNITS):
            for q in range(QUADS):
                m = device(0, yr, away(u, q), cr)[0]
                columns = pl.ds(pl.multiple_of(m * (LOCALS * OWN), LOCALS * OWN), LOCALS * OWN)
                turned = act[:, columns].T
                for owner in range(LOCALS):
                    dx = (owner % NX - x + NX) % NX
                    hi = owner // NX
                    kind = (1 - yr) * OWN_CLASS * ((hi + y_hi + 1) % NYHI) + yr * (1 + (hi + next_hi) % NYHI)
                    at_send[dx, kind, u, cr * QUADS + q] = turned[owner * OWN : (owner + 1) * OWN]
        return carry

    lax.fori_loop(0, NYLO * NCORE, transpose_pair, 0)
    for load in loads[1:]:
        load.wait()

    def ring_term(dx, kind, u, b):
        inputs = at_send[0, kind, u] if dx == 0 else at_recv[dx - 1, kind, u]
        grad = jnp.dot(inputs.reshape(ROWS, TOK), g[dx, b], preferred_element_type=F32)
        return quantize_restore(grad)

    def own_terms(kind, carry):
        for u in range(UNITS):
            for b in range(HALVES):
                base[kind, u, b] = ring_term(0, kind, u, b)
        return carry

    pl.semaphore_wait(barrier, len(peers) + along(1))

    def g_copy(dx, b):
        return remote(g.at[0, b], g.at[dx, b], g_ss.at[dx - 1, b], g_rs.at[dx - 1, b], device(dx, 0, 0, 0))

    def a_copy(dx, kind, u):
        return remote(
            at_send.at[dx, kind, u], at_recv.at[dx - 1, kind, u],
            a_ss.at[dx - 1, kind, u], a_rs.at[dx - 1, kind, u], device(dx, 0, 0, 0),
        )

    def y_copy(kind, step, u, halves):
        part = pl.ds(halves[0], len(halves))
        sem = u * HALVES + halves[0]
        return remote(
            y_send.at[kind, u, part], y_recv.at[kind, u, part],
            y_ss.at[kind, sem], y_rs.at[kind, sem], device(0, step, 0, 0),
        )

    def d_copy(u):
        return remote(d_send.at[u], d_recv.at[u], d_ss.at[u], d_rs.at[u], device(0, 0, 0, 1))

    def z_copy(u, q, dz):
        return remote(z_send.at[u, q], z_recv.at[dz], z_ss.at[u, q], z_rs.at[dz], device(0, 0, dz, 0))

    def w_copy(i):
        dy, dx = 2 * ((i + 1) // NX), (i + 1) % NX
        mine = pl.ds(pl.multiple_of(local * OWN, OWN), OWN)
        return remote(weight, weight_out.at[mine], w_ss.at[i], w_rs.at[i], device(dx, dy, 0, 0))

    across = (2, 1, 3)

    def send_inputs(kind, u):
        for dx in across:
            a_copy(dx, kind, u).start()

    for dx in across:
        g_copy(dx, 0).start()
    for u in range(FIRST):
        send_inputs(0, u)
    for dx in across:
        g_copy(dx, 1).start()
    for kind, u in LATER:
        send_inputs(kind, u)
    tell(0)
    lax.fori_loop(0, CLASSES, own_terms, 0)

    def ring_sum(kind, u, b):
        total = base[kind, u, b]
        for dx in range(1, NX):
            total = total + ring_term(dx, kind, u, b)
        return total

    def first_rows(u, b):
        y_send[0, u, b] = ring_sum(0, u, b).astype(BF16)
        y_copy(0, STEP[0], u, (b,)).start()

    for b in range(HALVES):
        for dx in across:
            g_copy(dx, b).wait_recv()
        heard(b)
        tell(b + 1)
        for u in range(FIRST):
            if b == 0:
                for dx in across:
                    a_copy(dx, 0, u).wait_recv()
            first_rows(u, b)
    def next_rows(i, carry):
        kind, u = 1 + i % 2, i // 2
        for dx in across:
            a_copy(dx, kind, u).wait_recv()
        sums = [ring_sum(kind, u, b) for b in range(HALVES)]
        for b in range(HALVES):
            y_send[kind, u, b] = sums[b].astype(BF16)
        y_copy(kind, 2 * kind - 1, u, BOTH).start()
        return carry

    lax.fori_loop(0, 2 * FIRST, next_rows, 0)
    for u in range(FIRST, UNITS):
        for dx in across:
            a_copy(dx, 0, u).wait_recv()
        for b in range(HALVES):
            first_rows(u, b)

    def own_node(u):
        for dx in across:
            a_copy(dx, OWN_CLASS, u).wait_recv()
        for b in range(HALVES):
            y_copy(0, STEP[0], u, (b,)).wait_recv()
        sums = [ring_sum(OWN_CLASS, u, b) + y_recv[0, u, b].astype(F32) for b in range(HALVES)]
        sums = [quantize_restore(total) for total in sums]
        for b in range(HALVES):
            base[OWN_CLASS, u, b] = sums[b]

    def next_node(u):
        for kind in (1, 2):
            y_copy(kind, STEP[kind], u, BOTH).wait_recv()
        for b in range(HALVES):
            both = quantize_restore(y_recv[1, u, b].astype(F32) + y_recv[2, u, b].astype(F32))
            both = both + base[OWN_CLASS, u, b]
            keep[u, b] = both[:KEEP]
            d_send[u, b] = both[KEEP:]
        d_copy(u).start()

    def to_owners(u):
        d_copy(u).wait_recv()
        for q in range(QUADS):
            rows = pl.ds(q * OWN, OWN)
            pair = keep[u, :, rows] + d_recv[u, :, rows]
            for b in range(HALVES):
                if u * QUADS + q == LAST:
                    own_sum[:, b * BLOCK : (b + 1) * BLOCK] = pair[b]
                else:
                    z_send[u, q, :, b * BLOCK : (b + 1) * BLOCK] = pair[b].astype(BF16)
            if u * QUADS + q != LAST:
                z_copy(u, q, away(u, q)).start()

    for u in range(UNITS):
        own_node(u)
        if u >= 2:
            @pl.when(core == 1)
            def _(u=u):
                to_owners(u - 2)

        next_node(u)
        if u == 0:
            heard(2)

        @pl.when(core == 0)
        def _(u=u):
            to_owners(u)

        if u == 0:
            lax.fori_loop(2 * FIRST, 2 * UNITS, next_rows, 0)

    @pl.when(core == 1)
    def _():
        for u in range(2, UNITS):
            to_owners(u)

    total = own_sum[...]
    for dz in range(1, NZ):
        z_copy(0, 0, dz).wait_recv()
        total = total + z_recv[dz].astype(F32)
    grad = total / (NODES * LOCALS)
    first_now = 0.9 * first[...] + 0.1 * grad
    second_now = 0.95 * second[...] + 0.05 * grad * grad
    update = first_now / (1.0 - 0.9**10) / (jnp.sqrt(second_now / (1.0 - 0.95**10)) + 1e-08)
    weight[...] = (master[...] - 0.01 * update).astype(BF16)
    for i in (5, 4, 6, 3, 1, 0, 2):
        w_copy(i).start()
    weight_out[pl.ds(pl.multiple_of(local * OWN, OWN), OWN)] = weight[...]
    first_out[...] = first_now
    second_out[...] = second_now

    for dx in across:
        for b in range(HALVES):
            g_copy(dx, b).wait_send()

    def drain(u, carry):
        for kind in range(CLASSES):
            for dx in across:
                a_copy(dx, kind, u).wait_send()
        for b in range(HALVES):
            y_copy(0, STEP[0], u, (b,)).wait_send()
        for kind in (1, 2):
            y_copy(kind, STEP[kind], u, BOTH).wait_send()
        d_copy(u).wait_send()
        return carry

    lax.fori_loop(0, UNITS, drain, 0)
    for u in range(UNITS):
        for q in range(QUADS):
            if u * QUADS + q != LAST:
                z_copy(u, q, away(u, q)).wait_send()
    for i in range(LOCALS - 1):
        w_copy(i).wait_send()
    for i in range(LOCALS - 1):
        w_copy(i).wait_recv()


def hand_out(weight, first, second, weight_out, first_out, second_out, sem):
    copies = [
        pltpu.make_async_copy(weight, weight_out, sem.at[0]),
        pltpu.make_async_copy(first, first_out, sem.at[1]),
        pltpu.make_async_copy(second, second_out, sem.at[2]),
    ]
    for copy in copies:
        copy.start()
    for copy in copies:
        copy.wait()


def per_device(activations, out_grads, master, first_moment, second_moment):
    anywhere = pl.BlockSpec(memory_space=pl.ANY)
    dma = pltpu.SemaphoreType.DMA
    vmem = pltpu.VMEM
    results = (
        jax.ShapeDtypeStruct((LOCALS * OWN, COLS), BF16),
        jax.ShapeDtypeStruct((OWN, COLS), F32),
        jax.ShapeDtypeStruct((OWN, COLS), F32),
    )
    arguments = (activations, out_grads, master, first_moment, second_moment)
    made = pl.pallas_call(
        kernel,
        out_shape=tuple(vmem(result.shape, result.dtype) for result in results),
        in_specs=[pl.BlockSpec(memory_space=pltpu.HBM)] * 5,
        out_specs=(pl.BlockSpec(memory_space=vmem),) * 3,
        scratch_shapes=[
            vmem((TOK, NODES * LOCALS * OWN), BF16),
            vmem((NX, CLASSES, UNITS, SLOTS, OWN, TOK), BF16),
            vmem((NX - 1, CLASSES, UNITS, SLOTS, OWN, TOK), BF16),
            vmem((NX, HALVES, TOK, BLOCK), BF16),
            vmem((CLASSES, UNITS, HALVES, ROWS, BLOCK), F32),
            vmem((CLASSES - 1, UNITS, HALVES, ROWS, BLOCK), BF16),
            vmem((CLASSES - 1, UNITS, HALVES, ROWS, BLOCK), BF16),
            vmem((UNITS, HALVES, KEEP, BLOCK), F32),
            vmem((UNITS, HALVES, KEEP, BLOCK), F32),
            vmem((UNITS, HALVES, KEEP, BLOCK), F32),
            vmem((UNITS, QUADS, OWN, COLS), BF16),
            vmem((NZ, OWN, COLS), BF16),
            vmem((OWN, COLS), F32),
            vmem((OWN, COLS), F32),
            vmem((OWN, COLS), F32),
            vmem((OWN, COLS), F32),
            vmem((OWN, COLS), BF16),
            dma((4 + HALVES,)),
            dma((NX - 1, HALVES)),
            dma((NX - 1, HALVES)),
            dma((NX - 1, CLASSES, UNITS)),
            dma((NX - 1, CLASSES, UNITS)),
            dma((CLASSES - 1, UNITS * HALVES)),
            dma((CLASSES - 1, UNITS * HALVES)),
            dma((UNITS,)),
            dma((UNITS,)),
            dma((UNITS, QUADS)),
            dma((NZ,)),
            dma((LOCALS - 1,)),
            dma((LOCALS - 1,)),
            pltpu.SemaphoreType.REGULAR((len(REACH),)),
        ],
        compiler_params=pltpu.CompilerParams(
            collective_id=0, has_side_effects=True, vmem_limit_bytes=16 * 1024 * 1024
        ),
    )(*(pltpu.with_memory_space_constraint(argument, pltpu.HBM) for argument in arguments))
    return pl.pallas_call(
        hand_out,
        out_shape=results,
        in_specs=[pl.BlockSpec(memory_space=vmem)] * 3,
        out_specs=(anywhere,) * 3,
        scratch_shapes=[dma((3,))],
        compiler_params=pltpu.CompilerParams(vmem_limit_bytes=1024 * 1024),
    )(*made)


def solution(mesh):
    rows = P(("node", "local"), None)
    return jax.shard_map(
        per_device,
        mesh=mesh,
        in_specs=(rows,) * 5,
        out_specs=(P("node", None), rows, rows),
        check_vma=False,
    )
```

```python
import jax
import jax.numpy as jnp
from jax import lax
from jax.experimental import pallas as pl
from jax.experimental.pallas import tpu as pltpu
from jax.sharding import PartitionSpec as P

BLOCK = 256
MESH = pl.DeviceIdType.MESH
F32 = jnp.float32
BF16 = jnp.bfloat16

NX, NY, NZ, NCORE, NYLO, NYHI = 4, 4, 8, 2, 2, 2
NODES, LOCALS = 32, 8
OWN = 16
TOK = 128
COLS = 512
HALVES = COLS // BLOCK
UNITS = 4
QUADS = 2
LAST = NZ - 1
CLASSES = 4
STEP = (2, 1, 3, 0)
OWN_CLASS = 3
FIRST = 2
LATER = ((1, 0), (2, 0), (3, 0), (1, 1), (2, 1), (0, 2), (0, 3), (1, 2), (2, 2), (1, 3), (2, 3), (3, 1), (3, 2), (3, 3))
BOTH = tuple(range(HALVES))
SLOTS = NCORE * QUADS
ROWS = SLOTS * OWN
KEEP = ROWS // NCORE
REACH = (1, 2, 4)


def quantize_restore(values):
    largest = jnp.max(jnp.abs(values), axis=1, keepdims=True)
    scale = (largest + 1e-06) / 127.0
    payload = (values * (1.0 / scale)).astype(BF16)
    return payload.astype(F32) * scale


def kernel(
    act_hbm, grads_hbm, master_hbm, first_hbm, second_hbm,
    weight_out, first_out, second_out,
    act, at_send, at_recv, g, base, y_send, y_recv, keep, d_send, d_recv, z_send, z_recv, own_sum,
    master, first, second, weight,
    load_sem, g_ss, g_rs, a_ss, a_rs, y_ss, y_rs, d_ss, d_rs, z_ss, z_rs, w_ss, w_rs, hop_sem,
):
    node = lax.axis_index("node")
    local = lax.axis_index("local")
    core = node % NCORE
    z = (node // NCORE) % NZ
    x = local % NX
    y_hi = local // NX
    y = y_hi * NYLO + node // (NCORE * NZ)

    def device(dx, dy, dz, dc):
        to_y = (y + dy) % NY
        to_node = ((to_y % NYLO) * NZ + (z + dz) % NZ) * NCORE + (core + dc) % NCORE
        return to_node, (to_y // NYLO) * NX + (x + dx) % NX

    def away(u, q):
        place = u * QUADS + q
        return 0 if place == LAST else (place + (place + NZ - z) // NZ - z + NZ) % NZ

    def remote(src, dst, ss, rs, to):
        return pltpu.make_async_remote_copy(
            src_ref=src, dst_ref=dst, send_sem=ss, recv_sem=rs, device_id=to, device_id_type=MESH
        )

    peers = [
        *(device(dx, 0, 0, 0) for dx in (2, 1, 3)),
        *(device(0, dy, 0, 0) for dy in (2, 1, 3)),
        device(0, 0, 0, 1),
    ]
    def along(d):
        return (z + NZ - d) // NZ + 1 - (z + d) // NZ

    def signal_along(sem, d):
        @pl.when(z < NZ - d)
        def _():
            pl.semaphore_signal(sem, inc=1, device_id=device(0, 0, d, 0), device_id_type=MESH)

        @pl.when(z >= d)
        def _():
            pl.semaphore_signal(sem, inc=1, device_id=device(0, 0, NZ - d, 0), device_id_type=MESH)

    def tell(hop):
        signal_along(hop_sem.at[hop], REACH[hop])

    def heard(hop):
        pl.semaphore_wait(hop_sem.at[hop], along(REACH[hop]))

    loads = [
        pltpu.make_async_copy(act_hbm, act, load_sem.at[0]),
        *(
            pltpu.make_async_copy(grads_hbm.at[:, pl.ds(b * BLOCK, BLOCK)], g.at[0, b], load_sem.at[1 + b])
            for b in range(HALVES)
        ),
        pltpu.make_async_copy(master_hbm, master, load_sem.at[1 + HALVES]),
        pltpu.make_async_copy(first_hbm, first, load_sem.at[2 + HALVES]),
        pltpu.make_async_copy(second_hbm, second, load_sem.at[3 + HALVES]),
    ]
    loads[0].start()
    barrier = pltpu.get_barrier_semaphore()
    for peer in peers:
        pl.semaphore_signal(barrier, inc=1, device_id=peer, device_id_type=MESH)
    signal_along(barrier, 1)
    for load in loads[1:]:
        load.start()

    loads[0].wait()
    next_hi = ((y + 1) % NY) // NYLO

    def transpose_pair(i, carry):
        yr, cr = i // NCORE, i % NCORE
        for u in range(UNITS):
            for q in range(QUADS):
                m = device(0, yr, away(u, q), cr)[0]
                columns = pl.ds(pl.multiple_of(m * (LOCALS * OWN), LOCALS * OWN), LOCALS * OWN)
                turned = act[:, columns].T
                for owner in range(LOCALS):
                    dx = (owner % NX - x + NX) % NX
                    hi = owner // NX
                    kind = (1 - yr) * OWN_CLASS * ((hi + y_hi + 1) % NYHI) + yr * (1 + (hi + next_hi) % NYHI)
                    at_send[dx, kind, u, cr * QUADS + q] = turned[owner * OWN : (owner + 1) * OWN]
        return carry

    lax.fori_loop(0, NYLO * NCORE, transpose_pair, 0)
    for load in loads[1:]:
        load.wait()

    def ring_term(dx, kind, u, b):
        inputs = at_send[0, kind, u] if dx == 0 else at_recv[dx - 1, kind, u]
        grad = jnp.dot(inputs.reshape(ROWS, TOK), g[dx, b], preferred_element_type=F32)
        return quantize_restore(grad)

    def own_terms(kind, carry):
        for u in range(UNITS):
            for b in range(HALVES):
                base[kind, u, b] = ring_term(0, kind, u, b)
        return carry

    pl.semaphore_wait(barrier, len(peers) + along(1))

    def g_copy(dx, b):
        return remote(g.at[0, b], g.at[dx, b], g_ss.at[dx - 1, b], g_rs.at[dx - 1, b], device(dx, 0, 0, 0))

    def a_copy(dx, kind, u):
        return remote(
            at_send.at[dx, kind, u], at_recv.at[dx - 1, kind, u],
            a_ss.at[dx - 1, kind, u], a_rs.at[dx - 1, kind, u], device(dx, 0, 0, 0),
        )

    def y_copy(kind, step, u, halves):
        part = pl.ds(halves[0], len(halves))
        sem = u * HALVES + halves[0]
        return remote(
            y_send.at[kind, u, part], y_recv.at[kind, u, part],
            y_ss.at[kind, sem], y_rs.at[kind, sem], device(0, step, 0, 0),
        )

    def d_copy(u):
        return remote(d_send.at[u], d_recv.at[u], d_ss.at[u], d_rs.at[u], device(0, 0, 0, 1))

    def z_copy(u, q, dz):
        return remote(z_send.at[u, q], z_recv.at[dz], z_ss.at[u, q], z_rs.at[dz], device(0, 0, dz, 0))

    def w_copy(i):
        dy, dx = 2 * ((i + 1) // NX), (i + 1) % NX
        mine = pl.ds(pl.multiple_of(local * OWN, OWN), OWN)
        return remote(weight, weight_out.at[mine], w_ss.at[i], w_rs.at[i], device(dx, dy, 0, 0))

    across = (2, 1, 3)

    def send_inputs(kind, u):
        for dx in across:
            a_copy(dx, kind, u).start()

    for dx in across:
        g_copy(dx, 0).start()
    for u in range(FIRST):
        send_inputs(0, u)
    for dx in across:
        g_copy(dx, 1).start()
    for kind, u in LATER:
        send_inputs(kind, u)
    tell(0)
    lax.fori_loop(0, CLASSES, own_terms, 0)

    def ring_sum(kind, u, b):
        total = base[kind, u, b]
        for dx in range(1, NX):
            total = total + ring_term(dx, kind, u, b)
        return total

    def first_rows(u, b):
        y_send[0, u, b] = ring_sum(0, u, b).astype(BF16)
        y_copy(0, STEP[0], u, (b,)).start()

    for b in range(HALVES):
        for dx in across:
            g_copy(dx, b).wait_recv()
        heard(b)
        tell(b + 1)
        for u in range(FIRST):
            if b == 0:
                for dx in across:
                    a_copy(dx, 0, u).wait_recv()
            first_rows(u, b)
    def next_rows(i, carry):
        kind, u = 1 + i % 2, i // 2
        for dx in across:
            a_copy(dx, kind, u).wait_recv()
        sums = [ring_sum(kind, u, b) for b in range(HALVES)]
        for b in range(HALVES):
            y_send[kind, u, b] = sums[b].astype(BF16)
        y_copy(kind, 2 * kind - 1, u, BOTH).start()
        return carry

    lax.fori_loop(0, 2 * FIRST, next_rows, 0)
    for u in range(FIRST, UNITS):
        for dx in across:
            a_copy(dx, 0, u).wait_recv()
        for b in range(HALVES):
            first_rows(u, b)

    def own_node(u):
        for dx in across:
            a_copy(dx, OWN_CLASS, u).wait_recv()
        for b in range(HALVES):
            y_copy(0, STEP[0], u, (b,)).wait_recv()
        sums = [ring_sum(OWN_CLASS, u, b) + y_recv[0, u, b].astype(F32) for b in range(HALVES)]
        sums = [quantize_restore(total) for total in sums]
        for b in range(HALVES):
            base[OWN_CLASS, u, b] = sums[b]

    def next_node(u):
        for kind in (1, 2):
            y_copy(kind, STEP[kind], u, BOTH).wait_recv()
        for b in range(HALVES):
            both = quantize_restore(y_recv[1, u, b].astype(F32) + y_recv[2, u, b].astype(F32))
            both = both + base[OWN_CLASS, u, b]
            keep[u, b] = both[:KEEP]
            d_send[u, b] = both[KEEP:]
        d_copy(u).start()

    def to_owners(u):
        d_copy(u).wait_recv()
        for q in range(QUADS):
            rows = pl.ds(q * OWN, OWN)
            pair = keep[u, :, rows] + d_recv[u, :, rows]
            for b in range(HALVES):
                if u * QUADS + q == LAST:
                    own_sum[:, b * BLOCK : (b + 1) * BLOCK] = pair[b]
                else:
                    z_send[u, q, :, b * BLOCK : (b + 1) * BLOCK] = pair[b].astype(BF16)
            if u * QUADS + q != LAST:
                z_copy(u, q, away(u, q)).start()

    for u in range(UNITS):
        own_node(u)
        if u >= 2:
            @pl.when(core == 1)
            def _(u=u):
                to_owners(u - 2)

        next_node(u)
        if u == 0:
            heard(2)

        @pl.when(core == 0)
        def _(u=u):
            to_owners(u)

        if u == 0:
            lax.fori_loop(2 * FIRST, 2 * UNITS, next_rows, 0)

    @pl.when(core == 1)
    def _():
        for u in range(2, UNITS):
            to_owners(u)

    total = own_sum[...]
    for dz in range(1, NZ):
        z_copy(0, 0, dz).wait_recv()
        total = total + z_recv[dz].astype(F32)
    grad = total / (NODES * LOCALS)
    first_now = 0.9 * first[...] + 0.1 * grad
    second_now = 0.95 * second[...] + 0.05 * grad * grad
    update = first_now / (1.0 - 0.9**10) / (jnp.sqrt(second_now / (1.0 - 0.95**10)) + 1e-08)
    weight[...] = (master[...] - 0.01 * update).astype(BF16)
    for i in (5, 4, 6, 3, 1, 0, 2):
        w_copy(i).start()
    weight_out[pl.ds(pl.multiple_of(local * OWN, OWN), OWN)] = weight[...]
    first_out[...] = first_now
    second_out[...] = second_now

    for dx in across:
        for b in range(HALVES):
            g_copy(dx, b).wait_send()

    def drain(u, carry):
        for kind in range(CLASSES):
            for dx in across:
                a_copy(dx, kind, u).wait_send()
        for b in range(HALVES):
            y_copy(0, STEP[0], u, (b,)).wait_send()
        for kind in (1, 2):
            y_copy(kind, STEP[kind], u, BOTH).wait_send()
        d_copy(u).wait_send()
        return carry

    lax.fori_loop(0, UNITS, drain, 0)
    for u in range(UNITS):
        for q in range(QUADS):
            if u * QUADS + q != LAST:
                z_copy(u, q, away(u, q)).wait_send()
    for i in range(LOCALS - 1):
        w_copy(i).wait_send()
    for i in range(LOCALS - 1):
        w_copy(i).wait_recv()


def hand_out(weight, first, second, weight_out, first_out, second_out, sem):
    copies = [
        pltpu.make_async_copy(weight, weight_out, sem.at[0]),
        pltpu.make_async_copy(first, first_out, sem.at[1]),
        pltpu.make_async_copy(second, second_out, sem.at[2]),
    ]
    for copy in copies:
        copy.start()
    for copy in copies:
        copy.wait()


def per_device(activations, out_grads, master, first_moment, second_moment):
    anywhere = pl.BlockSpec(memory_space=pl.ANY)
    dma = pltpu.SemaphoreType.DMA
    vmem = pltpu.VMEM
    results = (
        jax.ShapeDtypeStruct((LOCALS * OWN, COLS), BF16),
        jax.ShapeDtypeStruct((OWN, COLS), F32),
        jax.ShapeDtypeStruct((OWN, COLS), F32),
    )
    arguments = (activations, out_grads, master, first_moment, second_moment)
    made = pl.pallas_call(
        kernel,
        out_shape=tuple(vmem(result.shape, result.dtype) for result in results),
        in_specs=[pl.BlockSpec(memory_space=pltpu.HBM)] * 5,
        out_specs=(pl.BlockSpec(memory_space=vmem),) * 3,
        scratch_shapes=[
            vmem((TOK, NODES * LOCALS * OWN), BF16),
            vmem((NX, CLASSES, UNITS, SLOTS, OWN, TOK), BF16),
            vmem((NX - 1, CLASSES, UNITS, SLOTS, OWN, TOK), BF16),
            vmem((NX, HALVES, TOK, BLOCK), BF16),
            vmem((CLASSES, UNITS, HALVES, ROWS, BLOCK), F32),
            vmem((CLASSES - 1, UNITS, HALVES, ROWS, BLOCK), BF16),
            vmem((CLASSES - 1, UNITS, HALVES, ROWS, BLOCK), BF16),
            vmem((UNITS, HALVES, KEEP, BLOCK), F32),
            vmem((UNITS, HALVES, KEEP, BLOCK), F32),
            vmem((UNITS, HALVES, KEEP, BLOCK), F32),
            vmem((UNITS, QUADS, OWN, COLS), BF16),
            vmem((NZ, OWN, COLS), BF16),
            vmem((OWN, COLS), F32),
            vmem((OWN, COLS), F32),
            vmem((OWN, COLS), F32),
            vmem((OWN, COLS), F32),
            vmem((OWN, COLS), BF16),
            dma((4 + HALVES,)),
            dma((NX - 1, HALVES)),
            dma((NX - 1, HALVES)),
            dma((NX - 1, CLASSES, UNITS)),
            dma((NX - 1, CLASSES, UNITS)),
            dma((CLASSES - 1, UNITS * HALVES)),
            dma((CLASSES - 1, UNITS * HALVES)),
            dma((UNITS,)),
            dma((UNITS,)),
            dma((UNITS, QUADS)),
            dma((NZ,)),
            dma((LOCALS - 1,)),
            dma((LOCALS - 1,)),
            pltpu.SemaphoreType.REGULAR((len(REACH),)),
        ],
        compiler_params=pltpu.CompilerParams(
            collective_id=0, has_side_effects=True, vmem_limit_bytes=16 * 1024 * 1024
        ),
    )(*(pltpu.with_memory_space_constraint(argument, pltpu.HBM) for argument in arguments))
    return pl.pallas_call(
        hand_out,
        out_shape=results,
        in_specs=[pl.BlockSpec(memory_space=vmem)] * 3,
        out_specs=(anywhere,) * 3,
        scratch_shapes=[dma((3,))],
        compiler_params=pltpu.CompilerParams(vmem_limit_bytes=1024 * 1024),
    )(*made)


def solution(mesh):
    rows = P(("node", "local"), None)
    return jax.shard_map(
        per_device,
        mesh=mesh,
        in_specs=(rows,) * 5,
        out_specs=(P("node", None), rows, rows),
        check_vma=False,
    )
```
